32 devices in a mesh: cp: 32 (over z, y, x, core).
Axes of the slice: x: 2, y: 2, z: 4, core: 2. Of those that a mesh axis runs over, the one named last changes fastest.
Arguments:
- x_seq: bfloat16 [1, 24576, 64, 64], P(None, 'cp')
- dt_seq: float32 [1, 24576, 64], P(None, 'cp')
- a_log: float32 [64], replicated
- b_proj: bfloat16 [1, 24576, 128], P(None, 'cp')
- c_proj: bfloat16 [1, 24576, 128], P(None, 'cp')
- d_skip: float32 [64], replicated
- s_init: float32 [1, 64, 64, 128], replicated
- dy_seq: bfloat16 [1, 24576, 64, 64], P(None, 'cp')
- ds_last: float32 [1, 64, 64, 128], replicated
Outputs:
- output 1: bfloat16 [1, 24576, 64, 64], P(None, 'cp')
- output 2: float32 [1, 24576, 64], P(None, 'cp')
- output 3: bfloat16 [1, 24576, 128], P(None, 'cp')
- output 4: bfloat16 [1, 24576, 128], P(None, 'cp')
- output 5: float32 [1, 64, 64, 128], replicated
- output 6: float32 [64], replicated
- output 7: float32 [64], replicated
All inputs are finite; a program needn't handle non-finite values.
Results may differ from the reference program's by a relative error of at most 0.001.
Values sent between devices are 32-bit elements.
A program may use at most 1 GiB of HBM per device.

```python
import functools
import math
import jax
import jax.numpy as jnp
from jax import lax

BATCH = 1
SEQ = 24576
HEADS = 64
HEAD_DIM = 64
STATE = 128
CHUNK = 256
SPAN_LEN = 768


def setup_inputs(seed: int = 0) -> dict:
    rng_keys = jax.random.split(jax.random.key(seed), 10)
    x_seq = jax.random.normal(rng_keys[0], (BATCH, SEQ, HEADS, HEAD_DIM), jnp.float32).astype(jnp.bfloat16)
    dt_seq = jax.nn.softplus(0.5 * jax.random.normal(rng_keys[1], (BATCH, SEQ, HEADS), jnp.float32)) * (1.7 / SPAN_LEN)
    a_log = jax.random.uniform(rng_keys[2], (HEADS,), jnp.float32, math.log(0.25), 0.0)
    b_proj = jax.random.normal(rng_keys[3], (BATCH, SEQ, STATE), jnp.float32).astype(jnp.bfloat16)
    c_proj = jax.random.normal(rng_keys[4], (BATCH, SEQ, STATE), jnp.float32).astype(jnp.bfloat16)
    d_skip = jax.random.uniform(rng_keys[5], (HEADS,), jnp.float32, 0.2, 0.6)
    s_init = jax.random.normal(rng_keys[6], (BATCH, HEADS, HEAD_DIM, STATE), jnp.float32) * (SPAN_LEN ** -0.5)
    row_scale = jax.random.uniform(rng_keys[7], (BATCH, SEQ, 1, 1), jnp.float32, 0.5, 1.5)
    dy_seq = (jax.random.normal(rng_keys[8], (BATCH, SEQ, HEADS, HEAD_DIM), jnp.float32) * row_scale).astype(jnp.bfloat16)
    ds_last = jax.random.normal(rng_keys[9], (BATCH, HEADS, HEAD_DIM, STATE), jnp.float32) * (0.7 * SPAN_LEN ** 0.5)
    return {'x_seq': x_seq, 'dt_seq': dt_seq, 'a_log': a_log, 'b_proj': b_proj, 'c_proj': c_proj, 'd_skip': d_skip, 's_init': s_init, 'dy_seq': dy_seq, 'ds_last': ds_last}


def chunk_step(carry_state, blk_in, neg_rate, d_skip):
    x_blk, dt_blk, b_blk, c_blk = blk_in
    cum_decay = jnp.cumsum(dt_blk * neg_rate, axis=1)
    u_blk = x_blk * dt_blk[..., None]
    gram_mat = jnp.einsum('btn,bsn->bts', c_blk, b_blk)
    blk_len = x_blk.shape[1]
    causal = (jnp.arange(blk_len)[:, None] >= jnp.arange(blk_len)[None, :])[None, :, :, None]
    log_diff = jnp.where(causal, cum_decay[:, :, None, :] - cum_decay[:, None, :, :], 0.0)
    mix_mat = jnp.where(causal, jnp.exp(log_diff), 0.0) * gram_mat[..., None]
    y_blk = jnp.einsum('btsh,bshp->bthp', mix_mat, u_blk)
    y_blk = y_blk + jnp.exp(cum_decay)[..., None] * jnp.einsum('bhpn,btn->bthp', carry_state, c_blk)
    y_blk = y_blk + d_skip[:, None] * x_blk
    tail_decay = jnp.exp(cum_decay[:, -1:, :] - cum_decay)
    new_state = jnp.exp(cum_decay[:, -1, :])[..., None, None] * carry_state + jnp.einsum('bsh,bshp,bsn->bhpn', tail_decay, u_blk, b_blk)
    return new_state, y_blk


def ssd_forward(x_seq, dt_seq, a_log, b_proj, c_proj, d_skip, s_init):
    n_batch = x_seq.shape[0]
    n_span = SEQ // SPAN_LEN
    per_span = SPAN_LEN // CHUNK
    neg_rate = -jnp.exp(a_log)
    inner_step = jax.checkpoint(functools.partial(chunk_step, neg_rate=neg_rate, d_skip=d_skip))

    def span_step(carry_state, span_in):
        return lax.scan(inner_step, carry_state, span_in)

    def split_seq(array_in):
        blocks = array_in.astype(jnp.float32).reshape((n_batch, n_span, per_span, CHUNK) + array_in.shape[2:])
        return jnp.moveaxis(blocks, 0, 2)

    seq_in = (split_seq(x_seq), split_seq(dt_seq), split_seq(b_proj), split_seq(c_proj))
    final_state, y_blocks = lax.scan(jax.checkpoint(span_step), s_init, seq_in)
    y_seq = jnp.moveaxis(y_blocks, 2, 0).reshape(x_seq.shape)
    return y_seq, final_state


def reference(x_seq, dt_seq, a_log, b_proj, c_proj, d_skip, s_init, dy_seq, ds_last):
    _, pull_back = jax.vjp(ssd_forward, x_seq, dt_seq, a_log, b_proj, c_proj, d_skip, s_init)
    grad_x, grad_dt, grad_alog, grad_b, grad_c, grad_skip, grad_init = pull_back((dy_seq.astype(jnp.float32), ds_last))
    return (grad_x, grad_dt, grad_b, grad_c, grad_init, grad_alog, grad_skip)
```

```python
import functools
import jax
import jax.numpy as jnp
from jax import lax
from jax.sharding import PartitionSpec as P
from jax.experimental import pallas as pl
from jax.experimental.pallas import tpu as pltpu

AXIS = 'cp'
HEADS, HD, N = 64, 64, 128
GH = 8
GR = GH * HD
T = 128
LOG2E = 1.4426950408889634
F32, BF16 = jnp.float32, jnp.bfloat16
MESH = pl.DeviceIdType.MESH


def mm(a, b):
    return lax.dot_general(a, b, (((1,), (0,)), ((), ())), preferred_element_type=F32)


def mm_nt(a, b):
    return lax.dot_general(a, b, (((1,), (1,)), ((), ())), preferred_element_type=F32)


def mm_tn(a, b):
    return lax.dot_general(a, b, (((0,), (0,)), ((), ())), preferred_element_type=F32)


def split2(v):
    hi = v.astype(BF16)
    return hi, (v - hi.astype(F32)).astype(BF16)


def split3(v):
    hi = v.astype(BF16)
    r = v - hi.astype(F32)
    mid = r.astype(BF16)
    return hi, mid, (r - mid.astype(F32)).astype(BF16)


def dot_tri(v, tri):
    hi, mid, lo = split3(v)
    return mm(hi, tri) + mm(mid, tri) + mm(lo, tri)


def tri_mask(upper):
    r = lax.broadcasted_iota(jnp.int32, (T, T), 0)
    c = lax.broadcasted_iota(jnp.int32, (T, T), 1)
    keep = (r <= c) if upper else (r >= c)
    return jnp.where(keep, 1.0, 0.0)


def summary_kernel(nb, x_ref, dy_ref, dt_ref, rate_ref, b_ref, c_ref,
                   s_ref, ds_ref, ld_ref, cum_ref, xw, yw):
    tri = tri_mask(True).astype(BF16)
    dt = dt_ref[...]
    a = dt * rate_ref[:, 0:1]
    cums, tots = [], []
    for i in range(nb):
        cum = dot_tri(a[:, i * T:(i + 1) * T], tri)
        cum_ref[:, i * T:(i + 1) * T] = cum
        cums.append(cum)
        tots.append(cum[:, T - 1:T])
    before = [jnp.zeros_like(tots[0])]
    for i in range(nb):
        before.append(before[-1] + tots[i])
    after = [jnp.zeros_like(tots[0])]
    for i in reversed(range(1, nb)):
        after.append(after[-1] + tots[i])
    after = after[::-1]
    ld_ref[...] = jnp.broadcast_to(before[nb], (GH, T))
    for i in range(nb):
        w_in = dt[:, i * T:(i + 1) * T] * jnp.exp2((tots[i] - cums[i]) + after[i])
        w_out = jnp.exp2(cums[i] + before[i])
        lo_off = nb * T + i * T
        for j in range(GH):
            rows = slice(j * HD, (j + 1) * HD)
            hi, lo = split2(x_ref[rows, i * T:(i + 1) * T].astype(F32) * w_in[j:j + 1, :])
            xw[rows, i * T:(i + 1) * T] = hi
            xw[rows, lo_off:lo_off + T] = lo
            hi, lo = split2(dy_ref[rows, i * T:(i + 1) * T].astype(F32) * w_out[j:j + 1, :])
            yw[rows, i * T:(i + 1) * T] = hi
            yw[rows, lo_off:lo_off + T] = lo
    bb = b_ref[...]
    cc = c_ref[...]
    s_ref[...] = mm(xw[...], jnp.concatenate([bb, bb], axis=0))
    ds_ref[...] = mm(yw[...], jnp.concatenate([cc, cc], axis=0))


def summaries(x_t, dy_t, dt_t, rate, b, c):
    seq = x_t.shape[1]
    nb = seq // T
    rows = x_t.shape[0]
    big = pl.BlockSpec((GR, seq), lambda g: (g, 0))
    head = pl.BlockSpec((GH, seq), lambda g: (g, 0))
    hd1 = pl.BlockSpec((GH, T), lambda g: (g, 0))
    full = pl.BlockSpec((seq, N), lambda g: (0, 0))
    st = pl.BlockSpec((GR, N), lambda g: (g, 0))
    return pl.pallas_call(
        functools.partial(summary_kernel, nb),
        grid=(rows // GR,),
        in_specs=[big, big, head, hd1, full, full],
        out_specs=[st, st, hd1, head],
        out_shape=[jax.ShapeDtypeStruct((rows, N), F32), jax.ShapeDtypeStruct((rows, N), F32),
                   jax.ShapeDtypeStruct((rows // HD, T), F32), jax.ShapeDtypeStruct((rows // HD, seq), F32)],
        scratch_shapes=[pltpu.VMEM((GR, 2 * seq), BF16), pltpu.VMEM((GR, 2 * seq), BF16)],
        compiler_params=pltpu.CompilerParams(dimension_semantics=("arbitrary",)),
        name="summary",
    )(x_t, dy_t, dt_t, rate, b, c)


def main_kernel(nb, ng, x_ref, dy_ref, dt_ref, cum_ref, rate_ref, skip_ref, s0_ref, dse_ref, b_ref, c_ref,
                dx_ref, ddt_ref, dal_ref, dsk_ref, db_ref, dc_ref,
                gram, dgram, db_acc, dc_acc, s_cur, ds_cur, xw, yw, d_u, y_in, dcum, xdu):
    g = pl.program_id(0)

    @pl.when(g == 0)
    def _():
        low = tri_mask(False)
        for i in range(nb):
            tok = slice(i * T, (i + 1) * T)
            gram[i] = mm_nt(c_ref[tok, :], b_ref[tok, :]) * low
            dgram[i] = jnp.zeros((T, T), F32)
        db_acc[...] = jnp.zeros_like(db_acc)
        dc_acc[...] = jnp.zeros_like(dc_acc)

    ds_cur[...] = dse_ref[...]
    s_cur[...] = s0_ref[...]

    @pl.loop(0, nb)
    def _(it):
        i = nb - 1 - it
        tok = pl.ds(pl.multiple_of(i * T, T), T)
        cum = cum_ref[:, tok]
        tot = cum[:, T - 1:T]
        e_in = jnp.exp2(tot - cum)
        e_out = jnp.exp2(cum)
        w_in = dt_ref[:, tok] * e_in
        for j in range(GH):
            rows = slice(j * HD, (j + 1) * HD)
            hi, lo = split2(x_ref[rows, tok].astype(F32) * w_in[j:j + 1, :])
            xw[i, rows, 0:T] = hi
            xw[i, rows, T:2 * T] = lo
            hi, lo = split2(dy_ref[rows, tok].astype(F32) * e_out[j:j + 1, :])
            yw[i, rows, 0:T] = hi
            yw[i, rows, T:2 * T] = lo
        ds_hi, ds_lo = split2(ds_cur[...])
        bb = b_ref[tok, :]
        cc = c_ref[tok, :]
        inter = mm_nt(jnp.concatenate([ds_hi, ds_lo], axis=1), jnp.concatenate([bb, bb], axis=1))
        x_hi = xw[i, :, 0:T]
        db_acc[tok, :] += mm_tn(jnp.concatenate([x_hi, xw[i, :, T:2 * T], x_hi], axis=0),
                                jnp.concatenate([ds_hi, ds_hi, ds_lo], axis=0))
        upd = mm(yw[i], jnp.concatenate([cc, cc], axis=0))
        e_tot = jnp.exp2(tot)
        for j in range(GH):
            rows = slice(j * HD, (j + 1) * HD)
            d_u[rows, tok] = inter[rows, :] * e_in[j:j + 1, :]
            ds_cur[rows, :] = ds_cur[rows, :] * e_tot[j:j + 1, :] + upd[rows, :]

    @pl.loop(0, nb)
    def _(i):
        tok = pl.ds(pl.multiple_of(i * T, T), T)
        cum = cum_ref[:, tok]
        tot = cum[:, T - 1:T]
        e_tot = jnp.exp2(tot)
        e_out = jnp.exp2(cum)
        dt = dt_ref[:, tok]
        s_hi, s_lo = split2(s_cur[...])
        bb = b_ref[tok, :]
        cc = c_ref[tok, :]
        y_in[...] = mm_nt(jnp.concatenate([s_hi, s_lo], axis=1), jnp.concatenate([cc, cc], axis=1))
        y_hi = yw[i, :, 0:T]
        dc_acc[tok, :] += mm_tn(jnp.concatenate([y_hi, yw[i, :, T:2 * T], y_hi], axis=0),
                                jnp.concatenate([s_hi, s_hi, s_lo], axis=0))
        upd = mm(xw[i], jnp.concatenate([bb, bb], axis=0))
        for j in range(GH):
            rows = slice(j * HD, (j + 1) * HD)
            s_cur[rows, :] = s_cur[rows, :] * e_tot[j:j + 1, :] + upd[rows, :]
        cum_c = jnp.transpose(cum)
        g_i = gram[i]
        for j in range(GH):
            rows = slice(j * HD, (j + 1) * HD)
            row = slice(j, j + 1)
            xb = x_ref[rows, tok]
            yb = dy_ref[rows, tok]
            xf = xb.astype(F32)
            yf = yb.astype(F32)
            dtr = dt[row, :]
            u_hi, u_lo = split2(xf * dtr)
            pair = mm_tn(jnp.concatenate([yb, yb], axis=0), jnp.concatenate([u_hi, u_lo], axis=0))
            lam = jnp.exp2(jnp.minimum(cum_c[:, j:j + 1] - cum[row, :], 0.0))
            dgram[i] += lam * pair
            m_hi, m_lo = split2(lam * g_i)
            du_b = mm(jnp.concatenate([yb, yb], axis=1), jnp.concatenate([m_hi, m_lo], axis=0))
            zero = jnp.zeros_like(u_lo)
            y2 = mm_nt(jnp.concatenate([jnp.concatenate([u_hi, u_hi], axis=1),
                                        jnp.concatenate([u_lo, zero], axis=1)], axis=0),
                       jnp.concatenate([m_hi, m_lo], axis=1))
            y = (y2[0:HD] + y2[HD:2 * HD]) + e_out[row, :] * y_in[rows, :]
            du = d_u[rows, tok] + du_b
            dx_ref[rows, tok] = (dtr * du + skip_ref[row, :] * yf).astype(BF16)
            xd = jnp.sum(xf * du, axis=0, keepdims=True)
            xdu[row, tok] = xd
            dcum[row, tok] = jnp.sum(yf * y, axis=0, keepdims=True) - dtr * xd
            sk = jnp.sum(xf * yf, axis=0, keepdims=True)

            @pl.when(i == 0)
            def _():
                dsk_ref[row, :] = sk

            @pl.when(i != 0)
            def _():
                dsk_ref[row, :] += sk

    for j in range(GH):
        rows = slice(j * HD, (j + 1) * HD)
        dal_ref[j:j + 1, :] = jnp.sum(dse_ref[rows, :] * s_cur[rows, :], axis=0, keepdims=True)
    run = jnp.sum(dal_ref[...], axis=1, keepdims=True)
    rate = rate_ref[:, T - 1:T] * (1.0 / LOG2E)
    low = tri_mask(False).astype(BF16)
    total = jnp.zeros((GH, T), F32)
    for i in reversed(range(nb)):
        tok = slice(i * T, (i + 1) * T)
        da = dot_tri(dcum[:, tok], low) + run
        run = da[:, 0:1]
        da = da * rate
        ddt_ref[:, tok] = xdu[:, tok] + da
        total = total + dt_ref[:, tok] * da
    dal_ref[...] = jnp.broadcast_to(jnp.sum(total, axis=1, keepdims=True), (GH, T))
    dsk_ref[...] = jnp.broadcast_to(jnp.sum(dsk_ref[...], axis=1, keepdims=True), (GH, T))

    @pl.when(g == ng - 1)
    def _():
        low_f = tri_mask(False)
        for i in range(nb):
            tok = slice(i * T, (i + 1) * T)
            bb = b_ref[tok, :]
            cc = c_ref[tok, :]
            hi, lo = split2(dgram[i] * low_f)
            dc_ref[tok, :] = (dc_acc[tok, :] + (mm(hi, bb) + mm(lo, bb))).astype(BF16)
            db_ref[tok, :] = (db_acc[tok, :] + (mm_tn(hi, cc) + mm_tn(lo, cc))).astype(BF16)


def main_grads(x_t, dy_t, dt_t, cum, rate, skip, s0, dse, b, c):
    rows, seq = x_t.shape
    nb, ng = seq // T, rows // GR
    big = pl.BlockSpec((GR, seq), lambda g: (g, 0))
    head = pl.BlockSpec((GH, seq), lambda g: (g, 0))
    hd1 = pl.BlockSpec((GH, T), lambda g: (g, 0))
    full = pl.BlockSpec((seq, N), lambda g: (0, 0))
    st = pl.BlockSpec((GR, N), lambda g: (g, 0))
    sd = jax.ShapeDtypeStruct
    return pl.pallas_call(
        functools.partial(main_kernel, nb, ng),
        grid=(ng,),
        in_specs=[big, big, head, head, hd1, hd1, st, st, full, full],
        out_specs=[big, head, hd1, hd1, full, full],
        out_shape=[sd((rows, seq), BF16), sd((rows // HD, seq), F32), sd((rows // HD, T), F32),
                   sd((rows // HD, T), F32), sd((seq, N), BF16), sd((seq, N), BF16)],
        scratch_shapes=[pltpu.VMEM((nb, T, T), F32), pltpu.VMEM((nb, T, T), F32),
                        pltpu.VMEM((seq, N), F32), pltpu.VMEM((seq, N), F32),
                        pltpu.VMEM((GR, N), F32), pltpu.VMEM((GR, N), F32),
                        pltpu.VMEM((nb, GR, 2 * T), BF16), pltpu.VMEM((nb, GR, 2 * T), BF16),
                        pltpu.VMEM((GR, seq), F32), pltpu.VMEM((GR, T), F32),
                        pltpu.VMEM((GH, seq), F32), pltpu.VMEM((GH, seq), F32)],
        compiler_params=pltpu.CompilerParams(dimension_semantics=("arbitrary",)),
        name="main_grads",
    )(x_t, dy_t, dt_t, cum, rate, skip, s0, dse, b, c)


def link_kernel(sp, dsp, ld, s_init, ds_last, start, end, first,
                r_s, r_ds, r_ld, c_s, c_ds, c_ld, p_s, p_ds, p_ld, t_s, t_ds, t_ld, z_b, z_ld,
                b_s, b_ds, a_s, a_ds, o_s, o_ds, f_own, f_all,
                send0, recv0, send1, recv1, send2, recv2, send3, recv3, send4, recv4, send5, recv5):
    me = lax.axis_index(AXIS)
    core = lax.rem(me, 2)
    chip = lax.rem(me // 2, 4)
    z = me // 8
    partner = z * 8 + chip * 2 + (1 - core)

    def at_chip(c):
        return z * 8 + c * 2 + core

    def at_z(zz):
        return zz * 8 + chip * 2 + core

    peers = [partner] + [at_chip(lax.rem(chip + r, 4)) for r in (1, 2, 3)] + [at_z(lax.rem(z + r, 4)) for r in (1, 2, 3)]
    barrier = pltpu.get_barrier_semaphore()
    for p in peers:
        pl.semaphore_signal(barrier, inc=1, device_id=(p,), device_id_type=MESH)
    pl.semaphore_wait(barrier, len(peers))

    def rcopy(src, dst, ssem, rsem, dev):
        return pltpu.make_async_remote_copy(src_ref=src, dst_ref=dst, send_sem=ssem, recv_sem=rsem,
                                            device_id=(dev,), device_id_type=MESH)

    h0 = core * 32
    o0 = (1 - core) * 32
    st0 = [rcopy(sp.at[pl.ds(o0, 32)], r_s, send0.at[0], recv0.at[0], partner),
           rcopy(dsp.at[pl.ds(o0, 32)], r_ds, send0.at[1], recv0.at[1], partner),
           rcopy(ld, r_ld, send0.at[2], recv0.at[2], partner)]
    for cp in st0:
        cp.start()
    for cp in st0:
        cp.wait()

    @pl.loop(0, 32)
    def _(h):
        hh = h0 + h
        own = jnp.exp2(ld[pl.ds(hh, 1), :])
        oth = jnp.exp2(r_ld[pl.ds(hh, 1), :])
        c_ld[pl.ds(h, 1), :] = ld[pl.ds(hh, 1), :] + r_ld[pl.ds(hh, 1), :]

        @pl.when(core == 0)
        def _():
            c_s[h] = sp[hh] * oth + r_s[h]
            c_ds[h] = dsp[hh] + own * r_ds[h]

        @pl.when(core == 1)
        def _():
            c_s[h] = r_s[h] * own + sp[hh]
            c_ds[h] = r_ds[h] + oth * dsp[hh]

    def copies1(c_dst, c_slot):
        part = pl.ds(c_dst * 8, 8)
        dev = at_chip(c_dst)
        return [rcopy(c_s.at[part], p_s.at[c_slot], send1.at[0, c_dst], recv1.at[0, c_slot], dev),
                rcopy(c_ds.at[part], p_ds.at[c_slot], send1.at[1, c_dst], recv1.at[1, c_slot], dev),
                rcopy(c_ld.at[part], p_ld.at[c_slot], send1.at[2, c_dst], recv1.at[2, c_slot], dev)]

    for r in (2, 1, 3):
        for cp in copies1(lax.rem(chip + r, 4), chip):
            cp.start()

    @pl.loop(0, 8)
    def _(h):
        p_s[chip, h] = c_s[chip * 8 + h]
        p_ds[chip, h] = c_ds[chip * 8 + h]
    p_ld[chip] = c_ld[pl.ds(pl.multiple_of(chip * 8, 8), 8), :]
    for r in (1, 2, 3):
        other = lax.rem(chip + r, 4)
        for cp in copies1(other, other):
            cp.wait_recv()

    t_ld[...] = p_ld[0] + p_ld[1] + p_ld[2] + p_ld[3]

    @pl.loop(0, 8)
    def _(h):
        d = [jnp.exp2(p_ld[c, pl.ds(h, 1), :]) for c in range(4)]
        acc = p_s[0, h]
        for c in (1, 2, 3):
            acc = acc * d[c] + p_s[c, h]
        t_s[h] = acc
        acc = p_ds[3, h]
        for c in (2, 1, 0):
            acc = acc * d[c] + p_ds[c, h]
        t_ds[h] = acc

    def copies2(z_dst, z_slot):
        return (rcopy(t_s, z_b.at[z_slot], send2.at[0, z_dst], recv2.at[0, z_slot], at_z(z_dst)),
                rcopy(t_ds, z_b.at[z_slot], send2.at[0, z_dst], recv2.at[0, z_slot], at_z(z_dst)),
                rcopy(t_ld, z_ld.at[z_slot], send2.at[1, z_dst], recv2.at[1, z_slot], at_z(z_dst)))

    for r in (1, 2, 3):
        zz = lax.rem(z + r, 4)
        right, left, dec = copies2(zz, z)

        @pl.when(zz > z)
        def _():
            right.start()

        @pl.when(zz < z)
        def _():
            left.start()
        dec.start()
    for r in (1, 2, 3):
        zz = lax.rem(z + r, 4)
        right, left, dec = copies2(zz, zz)
        right.wait_recv()
        dec.wait_recv()

    part8 = h0 + chip * 8

    @pl.loop(0, 8)
    def _(h):
        b_s[0, h] = s_init[part8 + h]
        b_ds[3, h] = ds_last[part8 + h]
        for zz in range(4):
            @pl.when(zz < z)
            def _():
                b_s[0, h] = b_s[0, h] * jnp.exp2(z_ld[zz, pl.ds(h, 1), :]) + z_b[zz, h]
        for zz in (3, 2, 1):
            @pl.when(zz > z)
            def _():
                b_ds[3, h] = b_ds[3, h] * jnp.exp2(z_ld[zz, pl.ds(h, 1), :]) + z_b[zz, h]
        d = [jnp.exp2(p_ld[c, pl.ds(h, 1), :]) for c in range(4)]
        acc = b_s[0, h]
        for c in (0, 1, 2):
            acc = acc * d[c] + p_s[c, h]
            b_s[c + 1, h] = acc
        acc = b_ds[3, h]
        for c in (3, 2, 1):
            acc = acc * d[c] + p_ds[c, h]
            b_ds[c - 1, h] = acc
        f_own[h] = acc * d[0] + p_ds[0, h]

    def copies3(c_dst, c_slot):
        dev = at_chip(c_dst)
        return [rcopy(b_s.at[c_dst], a_s.at[c_slot], send3.at[0, c_dst], recv3.at[0, c_slot], dev),
                rcopy(b_ds.at[c_dst], a_ds.at[c_slot], send3.at[1, c_dst], recv3.at[1, c_slot], dev)]

    for r in (2, 1, 3):
        for cp in copies3(lax.rem(chip + r, 4), chip):
            cp.start()

    def copy_f(zz):
        return rcopy(f_own, f_all.at[chip], send5.at[0, zz], recv5.at[0, chip], at_z(zz))

    @pl.when(z == 0)
    def _():
        for zz in (1, 2, 3):
            copy_f(zz).start()

        @pl.loop(0, 8)
        def _(h):
            f_all[chip, h] = f_own[h]

    @pl.loop(0, 8)
    def _(h):
        a_s[chip, h] = b_s[chip, h]
        a_ds[chip, h] = b_ds[chip, h]

    for r in (1, 2, 3):
        other = lax.rem(chip + r, 4)
        for cp in copies3(other, other):
            cp.wait_recv()

    def pair(h, c, hc):
        hh = h0 + h
        own = jnp.exp2(ld[pl.ds(hh, 1), :])
        oth = jnp.exp2(r_ld[pl.ds(hh, 1), :])

        @pl.when(core == 0)
        def _():
            start[hh] = a_s[c, hc]
            end[hh] = r_ds[h] + oth * a_ds[c, hc]
            o_s[h] = own * a_s[c, hc] + sp[hh]
            o_ds[h] = a_ds[c, hc]

        @pl.when(core == 1)
        def _():
            start[hh] = oth * a_s[c, hc] + r_s[h]
            end[hh] = a_ds[c, hc]
            o_s[h] = a_s[c, hc]
            o_ds[h] = dsp[hh] + own * a_ds[c, hc]

    for c in range(4):
        @pl.loop(0, 8)
        def _(hc):
            pair(c * 8 + hc, c, hc)

    mine = pl.ds(h0, 32)
    st4 = [rcopy(o_s, start.at[mine], send4.at[0], recv4.at[0], partner),
           rcopy(o_ds, end.at[mine], send4.at[1], recv4.at[1], partner)]
    for cp in st4:
        cp.start()

    @pl.when(z > 0)
    def _():
        copy_f(z).wait_recv()

    def copies5(c_dst, c_slot):
        return rcopy(f_all.at[chip], f_all.at[c_slot], send5.at[1, c_dst], recv5.at[1, c_slot], at_chip(c_dst))

    for r in (2, 1, 3):
        copies5(lax.rem(chip + r, 4), chip).start()
    for r in (1, 2, 3):
        other = lax.rem(chip + r, 4)
        copies5(other, other).wait_recv()

    for c in range(4):
        @pl.loop(0, 8)
        def _(hc):
            first[h0 + c * 8 + hc] = f_all[c, hc]
    last = [rcopy(f_all.at[c], first.at[pl.ds(h0 + c * 8, 8)], send5.at[2, c], recv5.at[2, c], partner) for c in range(4)]
    for cp in last:
        cp.start()
    for cp in last:
        cp.wait_recv()
    for cp in st4:
        cp.wait()
    for cp in last:
        cp.wait_send()
    for r in (1, 2, 3):
        other = lax.rem(chip + r, 4)
        for cp in copies1(other, chip) + copies3(other, chip) + [copies5(other, chip)]:
            cp.wait_send()
        zz = lax.rem(z + r, 4)
        right, left, dec = copies2(zz, z)
        right.wait_send()
        dec.wait_send()

    @pl.when(z == 0)
    def _():
        for zz in (1, 2, 3):
            copy_f(zz).wait_send()


def link_ranges(sp, dsp, ld, s_init, ds_last):
    vm = pl.BlockSpec(memory_space=pltpu.VMEM)
    st = (HD, N)
    V = pltpu.VMEM
    D = pltpu.SemaphoreType.DMA
    full = jax.ShapeDtypeStruct((HEADS,) + st, F32)
    return pl.pallas_call(
        link_kernel,
        in_specs=[vm] * 5,
        out_specs=[vm] * 3,
        out_shape=[full, full, full],
        scratch_shapes=[V((32,) + st, F32), V((32,) + st, F32), V((HEADS, N), F32),
                        V((32,) + st, F32), V((32,) + st, F32), V((32, N), F32),
                        V((4, 8) + st, F32), V((4, 8) + st, F32), V((4, 8, N), F32),
                        V((8,) + st, F32), V((8,) + st, F32), V((8, N), F32),
                        V((4, 8) + st, F32), V((4, 8, N), F32),
                        V((4, 8) + st, F32), V((4, 8) + st, F32),
                        V((4, 8) + st, F32), V((4, 8) + st, F32),
                        V((32,) + st, F32), V((32,) + st, F32),
                        V((8,) + st, F32), V((4, 8) + st, F32),
                        D((3,)), D((3,)), D((3, 4)), D((3, 4)), D((2, 4)), D((2, 4)),
                        D((2, 4)), D((2, 4)), D((2,)), D((2,)), D((3, 4)), D((3, 4))],
        compiler_params=pltpu.CompilerParams(collective_id=0, has_side_effects=True),
        name="link_ranges",
    )(sp, dsp, ld, s_init, ds_last)


def solution(mesh):
    tok4 = P(None, AXIS, None, None)
    tok3 = P(None, AXIS, None)

    def device_step(x_loc, dt_loc, a_log, b_loc, c_loc, d_skip, s_init, dy_loc, ds_last):
        seq = x_loc.shape[1]
        x_t = x_loc[0].transpose(1, 2, 0).reshape(HEADS * HD, seq)
        dy_t = dy_loc[0].transpose(1, 2, 0).reshape(HEADS * HD, seq)
        dt_t = dt_loc[0].T
        rate = jnp.broadcast_to((-jnp.exp(a_log) * LOG2E)[:, None], (HEADS, T))
        skip = jnp.broadcast_to(d_skip[:, None], (HEADS, T))
        b, c = b_loc[0], c_loc[0]
        sp, dsp, ld, cum = summaries(x_t, dy_t, dt_t, rate, b, c)
        st = (HEADS, HD, N)
        start, end, first = link_ranges(sp.reshape(st), dsp.reshape(st), ld, s_init[0], ds_last[0])
        dx, ddt, dal, dsk, db, dc = main_grads(x_t, dy_t, dt_t, cum, rate, skip, start.reshape(HEADS * HD, N),
                                               end.reshape(HEADS * HD, N), b, c)
        grad_x = dx.reshape(HEADS, HD, seq).transpose(2, 0, 1)[None]
        grad_alog, grad_skip = lax.psum((dal[:, 0], dsk[:, 0]), AXIS)
        return grad_x, ddt.T[None], db[None], dc[None], first[None], grad_alog, grad_skip

    return jax.shard_map(device_step, mesh=mesh,
                         in_specs=(tok4, tok3, P(), tok3, tok3, P(), P(), tok4, P()),
                         out_specs=(tok4, tok3, tok3, tok3, P(), P(), P()),
                         check_vma=False)
```

```python
import functools
import jax
import jax.numpy as jnp
from jax import lax
from jax.sharding import PartitionSpec as P
from jax.experimental import pallas as pl
from jax.experimental.pallas import tpu as pltpu

AXIS = 'cp'
HEADS, HD, N = 64, 64, 128
GH = 8
GR = GH * HD
T = 128
PIECE, SHARE, OWN, CHIPS, PLANES, QS = 32, 16, 4, 4, 4, 2
ALL_CHIPS = range(CHIPS)
LOG2E = 1.4426950408889634
F32, BF16 = jnp.float32, jnp.bfloat16
MESH = pl.DeviceIdType.MESH


def mm(a, b):
    return lax.dot_general(a, b, (((1,), (0,)), ((), ())), preferred_element_type=F32)


def mm_nt(a, b):
    return lax.dot_general(a, b, (((1,), (1,)), ((), ())), preferred_element_type=F32)


def mm_tn(a, b):
    return lax.dot_general(a, b, (((0,), (0,)), ((), ())), preferred_element_type=F32)


def cat0(*parts):
    return jnp.concatenate(parts, axis=0)


def cat1(*parts):
    return jnp.concatenate(parts, axis=1)


def sum0(v):
    return jnp.sum(v, axis=0, keepdims=True)


def sum1(v):
    return jnp.sum(v, axis=1, keepdims=True)


def blk(i, size):
    return slice(i * size, (i + 1) * size)


def row(v, j):
    return v[blk(j, 1), :]


def last_col(v):
    return v[:, T - 1:T]


def split2(v):
    hi = v.astype(BF16)
    return hi, (v - hi.astype(F32)).astype(BF16)


def split3(v):
    hi = v.astype(BF16)
    r = v - hi.astype(F32)
    mid = r.astype(BF16)
    return hi, mid, (r - mid.astype(F32)).astype(BF16)


def dot_tri(v, tri):
    hi, mid, lo = split3(v)
    return mm(hi, tri) + mm(mid, tri) + mm(lo, tri)


def tri_mask(upper):
    r = lax.broadcasted_iota(jnp.int32, (T, T), 0)
    c = lax.broadcasted_iota(jnp.int32, (T, T), 1)
    keep = (r <= c) if upper else (r >= c)
    return jnp.where(keep, 1.0, 0.0)


def neighbours():
    me = lax.axis_index(AXIS)
    core = lax.rem(me, 2)
    chip = lax.rem(me // 2, CHIPS)
    z = me // (2 * CHIPS)
    partner = me + 1 - 2 * core
    chips = [lax.rem(chip + r, CHIPS) for r in (2, 1, 3)]
    planes = [lax.rem(z + r, PLANES) for r in (1, 2, 3)]

    def at_chip(c):
        return me + 2 * (c - chip)

    def at_z(zz):
        return me + 2 * CHIPS * (zz - z)

    return core, chip, z, partner, chips, planes, at_chip, at_z


def greet(partner, chips, planes, at_chip, at_z):
    barrier = pltpu.get_barrier_semaphore()
    for p in [partner] + [at_chip(c) for c in chips] + [at_z(zz) for zz in planes]:
        pl.semaphore_signal(barrier, inc=1, device_id=(p,), device_id_type=MESH)


def met(chips, planes):
    pl.semaphore_wait(pltpu.get_barrier_semaphore(), 1 + len(chips) + len(planes))


def rcopy(src, dst, ssem, rsem, dev):
    return pltpu.make_async_remote_copy(src_ref=src, dst_ref=dst, send_sem=ssem, recv_sem=rsem,
                                        device_id=(dev,), device_id_type=MESH)


def each(copies, act):
    for cp in copies:
        getattr(cp, act)()


def link_steps(ng, sp, dsp, ld, s_init, ds_last, start, end, first, sp_out,
               r_s, r_ds, r_ld, c_s, c_ds, c_ld, p_s, p_ds, p_ld, t_s, t_ds, t_ld, z_b, z_ld,
               b_s, b_ds, a_s, a_ds, n_s, n_ds, o_s, o_ds, f_own, f_all,
               send0, recv0, send1, recv1, send2, recv2, send3, recv3, send4, recv4, send5, recv5, loc):
    core, chip, z, partner, chips, planes, at_chip, at_z = neighbours()
    mine, theirs = core * SHARE, (1 - core) * SHARE

    def hello():
        greet(partner, chips, planes, at_chip, at_z)

    def own_loads(q):
        part = pl.ds(q * PIECE + mine + chip * OWN, OWN)
        return [pltpu.make_async_copy(s_init.at[part], b_s.at[q, 0], loc.at[q, 0]),
                pltpu.make_async_copy(ds_last.at[part], b_ds.at[q, CHIPS - 1], loc.at[q, 1])]

    def copies0(q):
        part = pl.ds(q * PIECE + theirs, SHARE)
        logs = pl.ds(q * PIECE, PIECE)
        return [rcopy(sp.at[part], r_s.at[q], send0.at[q, 0], recv0.at[q, 0], partner),
                rcopy(dsp.at[part], r_ds.at[q], send0.at[q, 1], recv0.at[q, 1], partner),
                rcopy(ld.at[logs], r_ld.at[q], send0.at[q, 2], recv0.at[q, 2], partner)]

    def swap(q):
        if q == 0:
            met(chips, planes)
        each(copies0(q) + own_loads(q), "start")

    def copies1(q, c_dst, c_slot):
        part = pl.ds(c_dst * OWN, OWN)
        dev = at_chip(c_dst)
        return [rcopy(c_ld.at[q], p_ld.at[q, c_slot], send1.at[q, 2, c_dst], recv1.at[q, 2, c_slot], dev),
                rcopy(c_s.at[q, part], p_s.at[q, c_slot], send1.at[q, 0, c_dst], recv1.at[q, 0, c_slot], dev),
                rcopy(c_ds.at[q, part], p_ds.at[q, c_slot], send1.at[q, 1, c_dst], recv1.at[q, 1, c_slot], dev)]

    def decay(ref, q, h):
        return jnp.exp2(ref[q, pl.ds(h, 1), :])

    def pairs(q):
        each(copies0(q), "wait")
        c_ld[q] = ld[blk(q, PIECE), :] + r_ld[q]

        @pl.loop(0, SHARE)
        def _(h):
            hh = q * PIECE + mine + h
            own = jnp.exp2(ld[pl.ds(hh, 1), :])
            oth = decay(r_ld, q, mine + h)

            @pl.when(core == 0)
            def _():
                c_s[q, h] = sp[hh] * oth + r_s[q, h]
                c_ds[q, h] = dsp[hh] + own * r_ds[q, h]

            @pl.when(core == 1)
            def _():
                c_s[q, h] = r_s[q, h] * own + sp[hh]
                c_ds[q, h] = r_ds[q, h] + oth * dsp[hh]

        for c in chips:
            each(copies1(q, c, chip), "start")
        p_ld[q, chip] = c_ld[q]

        @pl.loop(0, OWN)
        def _(h):
            p_s[q, chip, h] = c_s[q, chip * OWN + h]
            p_ds[q, chip, h] = c_ds[q, chip * OWN + h]

    def copy2(q, kind, z_dst, z_slot):
        return rcopy((t_s, t_ds)[kind].at[q], z_b.at[q, z_slot], send2.at[q, 0, z_dst], recv2.at[q, 0, z_slot], at_z(z_dst))

    def copy2_ld(q, z_dst, z_slot):
        return rcopy(t_ld.at[q], z_ld.at[q, z_slot], send2.at[q, 1, z_dst], recv2.at[q, 1, z_slot], at_z(z_dst))

    def chip_decays(q, h):
        return [jnp.exp2(p_ld[q, c, pl.ds(mine + chip * OWN + h, 1), :]) for c in ALL_CHIPS]

    def z_decay(q, zz, h):
        return jnp.exp2(z_ld[q, zz, pl.ds(mine + chip * OWN + h, 1), :])

    def plane(q):
        for c in chips:
            each(copies1(q, c, c), "wait_recv")
        t_ld[q] = sum(p_ld[q, c] for c in ALL_CHIPS)

        @pl.loop(0, OWN)
        def _(h):
            d = chip_decays(q, h)
            acc = p_s[q, 0, h]
            for c in ALL_CHIPS[1:]:
                acc = acc * d[c] + p_s[q, c, h]
            t_s[q, h] = acc
            acc = p_ds[q, CHIPS - 1, h]
            for c in ALL_CHIPS[-2::-1]:
                acc = acc * d[c] + p_ds[q, c, h]
            t_ds[q, h] = acc

        for zz in planes:
            copy2_ld(q, zz, z).start()

            @pl.when(zz > z)
            def _():
                copy2(q, 0, zz, z).start()

            @pl.when(zz < z)
            def _():
                copy2(q, 1, zz, z).start()

    def copies3(q, c_dst, c_slot):
        dev = at_chip(c_dst)
        part = pl.ds(c_slot * OWN, OWN)
        return [rcopy(b_s.at[q, c_dst], a_s.at[q, part], send3.at[q, 0, c_dst], recv3.at[q, 0, c_slot], dev),
                rcopy(b_ds.at[q, c_dst], a_ds.at[q, part], send3.at[q, 1, c_dst], recv3.at[q, 1, c_slot], dev)]

    def copy_f(q, zz):
        return rcopy(f_own.at[q], f_all.at[q, pl.ds(chip * OWN, OWN)], send5.at[q, 0, zz], recv5.at[q, 0, chip], at_z(zz))

    def prefix(q):
        for zz in planes:
            copy2_ld(q, zz, zz).wait_recv()
            copy2(q, 0, zz, zz).wait_recv()
        each(own_loads(q), "wait")

        @pl.loop(0, OWN)
        def _(h):
            for zz in range(PLANES - 1):
                @pl.when(zz < z)
                def _():
                    b_s[q, 0, h] = b_s[q, 0, h] * z_decay(q, zz, h) + z_b[q, zz, h]
            for zz in range(PLANES)[:0:-1]:
                @pl.when(zz > z)
                def _():
                    b_ds[q, CHIPS - 1, h] = b_ds[q, CHIPS - 1, h] * z_decay(q, zz, h) + z_b[q, zz, h]
            d = chip_decays(q, h)
            acc = b_s[q, 0, h]
            for c in ALL_CHIPS[:-1]:
                acc = acc * d[c] + p_s[q, c, h]
                b_s[q, c + 1, h] = acc
            acc = b_ds[q, CHIPS - 1, h]
            for c in ALL_CHIPS[:0:-1]:
                acc = acc * d[c] + p_ds[q, c, h]
                b_ds[q, c - 1, h] = acc
            f_own[q, h] = acc * d[0] + p_ds[q, 0, h]
            a_s[q, chip * OWN + h] = b_s[q, chip, h]
            a_ds[q, chip * OWN + h] = b_ds[q, chip, h]

        for c in chips:
            each(copies3(q, c, chip), "start")

    def send_first():
        @pl.when(z == 0)
        def _():
            for q in range(QS):
                for zz in range(1, PLANES):
                    copy_f(q, zz).start()

                @pl.loop(0, OWN)
                def _(h):
                    f_all[q, chip * OWN + h] = f_own[q, h]

    def out_copies(q):
        part = pl.ds(q * PIECE + mine, SHARE)
        return [rcopy(o_s.at[q], start.at[part], send4.at[q, 0], recv4.at[q, 0], partner),
                rcopy(o_ds.at[q], end.at[part], send4.at[q, 1], recv4.at[q, 1], partner),
                pltpu.make_async_copy(n_s.at[q], start.at[part], loc.at[q, 2]),
                pltpu.make_async_copy(n_ds.at[q], end.at[part], loc.at[q, 3])]

    def halve(q):
        for c in chips:
            each(copies3(q, c, c), "wait_recv")

        @pl.loop(0, SHARE)
        def _(h):
            hh = q * PIECE + mine + h
            own = jnp.exp2(ld[pl.ds(hh, 1), :])
            oth = decay(r_ld, q, mine + h)

            @pl.when(core == 0)
            def _():
                n_s[q, h] = a_s[q, h]
                n_ds[q, h] = r_ds[q, h] + oth * a_ds[q, h]
                o_s[q, h] = own * a_s[q, h] + sp[hh]
                o_ds[q, h] = a_ds[q, h]

            @pl.when(core == 1)
            def _():
                n_s[q, h] = oth * a_s[q, h] + r_s[q, h]
                n_ds[q, h] = a_ds[q, h]
                o_s[q, h] = a_s[q, h]
                o_ds[q, h] = dsp[hh] + own * a_ds[q, h]

        each(out_copies(q), "start")

    def copy5(q, c_dst, c_slot):
        part = f_all.at[q, pl.ds(c_slot * OWN, OWN)]
        return rcopy(part, part, send5.at[q, 1, c_dst], recv5.at[q, 1, c_slot], at_chip(c_dst))

    def spread(q):
        @pl.when(z > 0)
        def _():
            copy_f(q, z).wait_recv()

        for c in chips:
            copy5(q, c, chip).start()

    def last(q):
        part = first.at[pl.ds(q * PIECE + mine, SHARE)]
        return [rcopy(f_all.at[q], part, send4.at[q, 2], recv4.at[q, 2], partner),
                pltpu.make_async_copy(f_all.at[q], part, loc.at[q, 4])]

    def sp_copy():
        return [pltpu.make_async_copy(sp, sp_out, loc.at[0, 5])]

    def finish():
        for q in range(QS):
            for c in chips:
                copy5(q, c, c).wait_recv()
            each(last(q), "start")
        for q in range(QS):
            each(out_copies(q), "wait")
            for c in chips:
                each(copies1(q, c, chip) + copies3(q, c, chip) + [copy5(q, c, chip)], "wait_send")
            for zz in planes:
                copy2(q, 0, zz, z).wait_send()
                copy2_ld(q, zz, z).wait_send()

            @pl.when(z == 0)
            def _():
                for zz in range(1, PLANES):
                    copy_f(q, zz).wait_send()
        each(sp_copy(), "wait")
        for q in range(QS):
            each(last(q), "wait")

    early = {0: [hello], 4: [functools.partial(swap, 0)], 6: [functools.partial(pairs, 0)],
             8: [functools.partial(swap, 1), lambda: each(sp_copy(), "start")]}
    late = [(0, 2, functools.partial(pairs, 1)), (1, 2, functools.partial(plane, 0)), (2, 5, functools.partial(plane, 1)),
            (3, 0, functools.partial(prefix, 0)), (4, 3, functools.partial(prefix, 1)), (4, 3, send_first),
            (5, 0, functools.partial(halve, 0)), (6, 2, functools.partial(halve, 1)), (6, 3, functools.partial(spread, 0)),
            (6, 5, functools.partial(spread, 1)), (7, 5, finish)]
    return early, late


def link_shapes():
    st = (HD, N)
    V = pltpu.VMEM
    D = pltpu.SemaphoreType.DMA

    def states(*lead):
        return V((QS,) + lead + st, F32)

    def logs(*lead):
        return V((QS,) + lead + (PIECE, N), F32)

    share, four, own = states(SHARE), states(CHIPS, OWN), states(OWN)
    three = D((QS, 3, CHIPS))
    two = D((QS, 2, CHIPS))
    return [share, share, logs(), share, share, logs(), four, four, logs(CHIPS), own, own, logs(), four, logs(PLANES),
            four, four, share, share, share, share, share, share, own, share,
            D((QS, 3)), D((QS, 3)), three, three, two, two, two, two, D((QS, 3)), D((QS, 3)), two, two, D((QS, 6))]


def local_kernel(nb, ng, x_ref, dy_ref, dt_ref, rate_ref, b_ref, c_ref, s_init, ds_last,
                 du_ref, ry_ref, db_ref, dc_ref, cum_out, start, end, first, sp_out,
                 gram, dgram, s_cur, ds_cur, xw, yw, y_in, u_in, rcol, cums, sp, dsp, ld, *link_scratch):
    step_id = pl.program_id(0)
    early, late = link_steps(ng, sp, dsp, ld, s_init, ds_last, start, end, first, sp_out, *link_scratch)
    for at, steps in early.items():
        @pl.when(step_id == at)
        def _():
            for step in steps:
                step()

    @pl.when(step_id < ng)
    def _():
        range_states(nb, step_id, x_ref, dy_ref, dt_ref, rate_ref, b_ref, c_ref, cum_out, cums, sp, dsp, ld, xw, yw)

    @pl.when(step_id >= ng)
    def _():
        local_group(nb, ng, step_id - ng, late, x_ref, dy_ref, dt_ref, b_ref, c_ref, du_ref, ry_ref, db_ref, dc_ref,
                    gram, dgram, s_cur, ds_cur, xw, yw, y_in, u_in, rcol, cums.at[step_id - ng])


def range_states(nb, g, x_ref, dy_ref, dt_ref, rate_ref, b_ref, c_ref, cum_out, cums, sp, dsp, ld, xw, yw):
    tri = tri_mask(True).astype(BF16)
    dt = dt_ref[...]
    a = dt * rate_ref[:, :1]
    cum, before = [], [jnp.zeros((GH, 1), F32)]
    for i in range(nb):
        v = dot_tri(a[:, blk(i, T)], tri)
        cums[g, :, blk(i, T)] = v
        cum_out[:, blk(i, T)] = v
        cum.append(v)
        before.append(before[-1] + last_col(v))
    ld[pl.ds(pl.multiple_of(g * GH, GH), GH), :] = jnp.broadcast_to(before[nb], (GH, T))
    after = jnp.zeros((GH, 1), F32)
    acc_s = jnp.zeros((GR, N), F32)
    acc_ds = jnp.zeros((GR, N), F32)
    for i in reversed(range(nb)):
        tok = blk(i, T)
        w_in = dt[:, tok] * jnp.exp2((last_col(cum[i]) - cum[i]) + after)
        w_out = jnp.exp2(cum[i] + before[i])
        after = after + last_col(cum[i])
        for j in range(GH):
            rows = blk(j, HD)
            xw[i, rows, :T], xw[i, rows, T:] = split2(x_ref[rows, tok].astype(F32) * row(w_in, j))
            yw[i, rows, :T], yw[i, rows, T:] = split2(dy_ref[rows, tok].astype(F32) * row(w_out, j))
        acc_s += mm(xw[i], cat0(b_ref[tok, :], b_ref[tok, :]))
        acc_ds += mm(yw[i], cat0(c_ref[tok, :], c_ref[tok, :]))
    for j in range(GH):
        sp[g * GH + j] = acc_s[blk(j, HD), :]
        dsp[g * GH + j] = acc_ds[blk(j, HD), :]


def local_group(nb, ng, g, late, x_ref, dy_ref, dt_ref, b_ref, c_ref, du_ref, ry_ref, db_ref, dc_ref,
                gram, dgram, s_cur, ds_cur, xw, yw, y_in, u_in, rcol, cum_ref):
    @pl.when(g == 0)
    def _():
        low = tri_mask(False)
        for i in range(nb):
            tok = blk(i, T)
            gram[i] = mm_nt(c_ref[tok, :], b_ref[tok, :]) * low
            dgram[i] = jnp.zeros((T, T), F32)
        db_ref[...] = jnp.zeros_like(db_ref)
        dc_ref[...] = jnp.zeros_like(dc_ref)
        rcol[...] = jnp.zeros_like(rcol)

    ds_cur[...] = jnp.zeros_like(ds_cur)
    s_cur[...] = jnp.zeros_like(s_cur)

    @pl.loop(0, nb)
    def _(i):
        tok = pl.ds(pl.multiple_of(i * T, T), T)
        cum = cum_ref[:, tok]
        w_in = dt_ref[:, tok] * jnp.exp2(last_col(cum) - cum)
        e_out = jnp.exp2(cum)
        for j in range(GH):
            rows = blk(j, HD)
            hi, lo = split2(x_ref[rows, tok].astype(F32) * row(w_in, j))
            xw[i, rows, :T] = hi
            xw[i, rows, T:] = lo
            hi, lo = split2(dy_ref[rows, tok].astype(F32) * row(e_out, j))
            yw[i, rows, :T] = hi
            yw[i, rows, T:] = lo
            du_ref[rows, tok] = jnp.zeros((HD, T), F32)

    @pl.loop(0, nb)
    def _(i):
        for at_g, at_i, step in late:
            @pl.when((g == at_g) & (i == at_i))
            def _():
                step()

        k = nb - 1 - i
        tok_k = pl.ds(pl.multiple_of(k * T, T), T)
        tok = pl.ds(pl.multiple_of(i * T, T), T)

        cum_k = cum_ref[:, tok_k]
        tot_k = last_col(cum_k)
        ds_hi, ds_lo = split2(ds_cur[...])
        b_k = b_ref[tok_k, :]
        c_k = c_ref[tok_k, :]
        u_in[...] = mm_nt(cat1(ds_hi, ds_lo), cat1(b_k, b_k))
        db2 = mm_tn(xw[k, :, :T], cat1(ds_hi, ds_lo))
        db_ref[tok_k, :] += db2[:, :N] + db2[:, N:] + mm_tn(xw[k, :, T:], ds_hi)
        upd_k = mm(yw[k], cat0(c_k, c_k))
        e_in = jnp.exp2(tot_k - cum_k)
        e_tot_k = jnp.exp2(tot_k)
        for j in range(GH):
            rows = blk(j, HD)
            du_ref[rows, tok_k] += u_in[rows, :] * row(e_in, j)
            ds_cur[rows, :] = ds_cur[rows, :] * row(e_tot_k, j) + upd_k[rows, :]

        cum = cum_ref[:, tok]
        e_tot = jnp.exp2(last_col(cum))
        e_out = jnp.exp2(cum)
        dt = dt_ref[:, tok]
        s_hi, s_lo = split2(s_cur[...])
        b_i = b_ref[tok, :]
        c_i = c_ref[tok, :]
        y_in[...] = mm_nt(cat1(s_hi, s_lo), cat1(c_i, c_i))
        dc2 = mm_tn(yw[i, :, :T], cat1(s_hi, s_lo))
        dc_ref[tok, :] += dc2[:, :N] + dc2[:, N:] + mm_tn(yw[i, :, T:], s_hi)
        upd = mm(xw[i], cat0(b_i, b_i))
        for j in range(GH):
            rows = blk(j, HD)
            s_cur[rows, :] = s_cur[rows, :] * row(e_tot, j) + upd[rows, :]
        cum_c = jnp.transpose(cum)
        g_i = gram[i]
        zero = jnp.zeros((HD, T), BF16)
        inter = []
        for j0 in range(0, GH, 2):
            y_t = jnp.transpose(dy_ref[pl.ds(j0 * HD, T), tok])
            u0, v0 = split2(x_ref[blk(j0, HD), tok].astype(F32) * row(dt, j0))
            u1, v1 = split2(x_ref[blk(j0 + 1, HD), tok].astype(F32) * row(dt, j0 + 1))
            pair = mm(cat1(y_t, y_t), cat1(cat0(u0, zero, v0, zero), cat0(zero, u1, zero, v1)))
            e_sum = None
            for j, p in ((j0, pair[:, :T]), (j0 + 1, pair[:, T:])):
                rows = blk(j, HD)
                lam = jnp.exp2(jnp.minimum(cum_c[:, blk(j, 1)] - row(cum, j), 0.0))
                e_sum = lam * p if e_sum is None else e_sum + lam * p
                m = lam * g_i
                rcol[:, blk(j, 1)] = sum1(m * p)
                m_hi, m_lo = split2(m)
                yb = dy_ref[rows, tok]
                du_ref[rows, tok] += mm(cat1(yb, yb), cat0(m_hi, m_lo))
                inter.append(sum0(yb.astype(F32) * y_in[rows, :]))
            dgram[i] += e_sum
        ry_ref[:, tok] = jnp.transpose(rcol[...])[:GH, :] + e_out * cat0(*inter)

    @pl.when(g == ng - 1)
    def _():
        low_f = tri_mask(False)
        for i in range(nb):
            tok = blk(i, T)
            bb = b_ref[tok, :]
            cc = c_ref[tok, :]
            hi, lo = split2(dgram[i] * low_f)
            dc_ref[tok, :] += mm(hi, bb) + mm(lo, bb)
            db_ref[tok, :] += mm_tn(hi, cc) + mm_tn(lo, cc)


def local_grads(x_t, dy_t, dt_t, rate, b, c, s_init, ds_last):
    rows, seq = x_t.shape
    nb, ng = seq // T, rows // GR
    big = pl.BlockSpec((GR, seq), lambda g: (lax.rem(g, ng), 0))
    head = pl.BlockSpec((GH, seq), lambda g: (lax.rem(g, ng), 0))
    hd1 = pl.BlockSpec((GH, T), lambda g: (lax.rem(g, ng), 0))
    big_o = pl.BlockSpec((GR, seq), lambda g: (jnp.maximum(g - ng, 0), 0))
    head_o = pl.BlockSpec((GH, seq), lambda g: (jnp.maximum(g - ng, 0), 0))
    cum_o = pl.BlockSpec((GH, seq), lambda g: (jnp.minimum(g, ng - 1), 0))
    full = pl.BlockSpec((seq, N), lambda g: (0, 0))
    anyw = pl.BlockSpec(memory_space=pl.ANY)
    sd = jax.ShapeDtypeStruct
    state = sd((HEADS, HD, N), F32)
    V = pltpu.VMEM
    sq, grp, wide = V((nb, T, T), F32), V((GR, N), F32), V((nb, GR, 2 * T), BF16)
    return pl.pallas_call(
        functools.partial(local_kernel, nb, ng),
        grid=(2 * ng,),
        in_specs=[big, big, head, hd1, full, full, anyw, anyw],
        out_specs=[big_o, head_o, full, full, cum_o, anyw, anyw, anyw, anyw],
        out_shape=[sd((rows, seq), F32), sd((rows // HD, seq), F32), sd((seq, N), F32), sd((seq, N), F32),
                   sd((rows // HD, seq), F32), state, state, state, state],
        scratch_shapes=[sq, sq, grp, grp, wide, wide, grp, grp, V((T, T), F32), V((ng, GH, seq), F32),
                        V((HEADS, HD, N), F32), V((HEADS, HD, N), F32), V((HEADS, N), F32)] + link_shapes(),
        compiler_params=pltpu.CompilerParams(dimension_semantics=("arbitrary",), collective_id=0, has_side_effects=True),
        name="local_grads",
    )(x_t, dy_t, dt_t, rate, b, c, s_init, ds_last)


T2 = 256


def join_kernel(nb, ng, x_ref, dy_ref, dt_ref, cum_ref, rate_ref, skip_ref, s0_ref, dse_ref, sp_ref, b_ref, c_ref,
                du_ref, ry_ref, dbl_ref, dcl_ref,
                dx_ref, ddt_ref, dal_ref, dsk_ref, db_ref, dc_ref,
                db_acc, dc_acc, ein, eout, xw, yw, s2, d2, y_in, u_in, dcum, xdu, skt):
    g = pl.program_id(0)

    @pl.when(g == 0)
    def _():
        db_acc[...] = dbl_ref[...]
        dc_acc[...] = dcl_ref[...]

    cums = [cum_ref[:, i * T:(i + 1) * T] for i in range(nb)]
    tots = [last_col(v) for v in cums]
    acc = jnp.zeros_like(tots[0])
    for i in range(nb):
        eout[:, i * T:(i + 1) * T] = jnp.exp2(cums[i] + acc)
        acc = acc + tots[i]
    e_tot = jnp.exp2(acc)
    acc = jnp.zeros_like(tots[0])
    for i in reversed(range(nb)):
        ein[:, i * T:(i + 1) * T] = jnp.exp2((tots[i] - cums[i]) + acc)
        acc = acc + tots[i]

    s_hi, s_lo = split2(s0_ref[...])
    d_hi, d_lo = split2(dse_ref[...])
    s2[...] = cat1(s_hi, s_lo)
    d2[...] = cat1(d_hi, d_lo)

    @pl.loop(0, nb * T // T2)
    def _(i):
        tok = pl.ds(pl.multiple_of(i * T2, T2), T2)
        bb = b_ref[tok, :]
        cc = c_ref[tok, :]
        y_in[...] = mm_nt(s2[...], cat1(cc, cc))
        u_in[...] = mm_nt(d2[...], cat1(bb, bb))
        dt = dt_ref[:, tok]
        e_in = ein[:, tok]
        e_out = eout[:, tok]
        w_in = dt * e_in
        xds, rys, sks = [], [], []
        for j in range(GH):
            rows = blk(j, HD)
            xf = x_ref[rows, tok].astype(F32)
            yf = dy_ref[rows, tok].astype(F32)
            du = du_ref[rows, tok] + row(e_in, j) * u_in[rows, :]
            dx_ref[rows, tok] = (row(dt, j) * du + skip_ref[blk(j, 1), :1] * yf).astype(BF16)
            xds.append(sum0(xf * du))
            rys.append(sum0(yf * y_in[rows, :]))
            sks.append(sum0(xf * yf))
            xw[rows, :T2], xw[rows, T2:] = split2(xf * row(w_in, j))
            yw[rows, :T2], yw[rows, T2:] = split2(yf * row(e_out, j))
        dc2 = mm_tn(yw[:, :T2], s2[...])
        dc_acc[tok, :] += dc2[:, :N] + dc2[:, N:] + mm_tn(yw[:, T2:], s2[:, :N])
        db2 = mm_tn(xw[:, :T2], d2[...])
        db_acc[tok, :] += db2[:, :N] + db2[:, N:] + mm_tn(xw[:, T2:], d2[:, :N])
        xd = cat0(*xds)
        xdu[:, tok] = xd
        dcum[:, tok] = ry_ref[:, tok] + e_out * cat0(*rys) - dt * xd
        skt[:, tok] = cat0(*sks)

    for j in range(GH):
        rows = blk(j, HD)
        dal_ref[j:j + 1, :] = jnp.sum(dse_ref[rows, :] * (sp_ref[rows, :] + row(e_tot, j) * s0_ref[rows, :]), axis=0, keepdims=True)
    run = jnp.sum(dal_ref[...], axis=1, keepdims=True)
    rate = rate_ref[...] * (1.0 / LOG2E)
    low = tri_mask(False).astype(BF16)
    total = jnp.zeros((GH, T), F32)
    for i in reversed(range(nb)):
        tok = blk(i, T)
        da = dot_tri(dcum[:, tok], low) + run
        run = da[:, 0:1]
        da = da * rate
        ddt_ref[:, tok] = xdu[:, tok] + da
        total = total + dt_ref[:, tok] * da
    dal_ref[...] = jnp.broadcast_to(jnp.sum(total, axis=1, keepdims=True), (GH, T))
    dsk_ref[...] = jnp.broadcast_to(jnp.sum(skt[...], axis=1, keepdims=True), (GH, T))

    @pl.when(g == ng - 1)
    def _():
        db_ref[...] = db_acc[...].astype(BF16)
        dc_ref[...] = dc_acc[...].astype(BF16)


def join_grads(x_t, dy_t, dt_t, cum, rate, skip, s0, dse, sp, b, c, du, ry, dbl, dcl):
    rows, seq = x_t.shape
    nb, ng = seq // T, rows // GR
    big = pl.BlockSpec((GR, seq), lambda g: (g, 0))
    head = pl.BlockSpec((GH, seq), lambda g: (g, 0))
    hd1 = pl.BlockSpec((GH, T), lambda g: (g, 0))
    full = pl.BlockSpec((seq, N), lambda g: (0, 0))
    st = pl.BlockSpec((GR, N), lambda g: (g, 0))
    sd = jax.ShapeDtypeStruct
    return pl.pallas_call(
        functools.partial(join_kernel, nb, ng),
        grid=(ng,),
        in_specs=[big, big, head, head, hd1, hd1, st, st, st, full, full, big, head, full, full],
        out_specs=[big, head, hd1, hd1, full, full],
        out_shape=[sd((rows, seq), BF16), sd((rows // HD, seq), F32), sd((rows // HD, T), F32),
                   sd((rows // HD, T), F32), sd((seq, N), BF16), sd((seq, N), BF16)],
        scratch_shapes=[pltpu.VMEM((seq, N), F32), pltpu.VMEM((seq, N), F32),
                        pltpu.VMEM((GH, seq), F32), pltpu.VMEM((GH, seq), F32),
                        pltpu.VMEM((GR, 2 * T2), BF16), pltpu.VMEM((GR, 2 * T2), BF16),
                        pltpu.VMEM((GR, 2 * N), BF16), pltpu.VMEM((GR, 2 * N), BF16),
                        pltpu.VMEM((GR, T2), F32), pltpu.VMEM((GR, T2), F32),
                        pltpu.VMEM((GH, seq), F32), pltpu.VMEM((GH, seq), F32), pltpu.VMEM((GH, seq), F32)],
        compiler_params=pltpu.CompilerParams(dimension_semantics=("arbitrary",)),
        name="join_grads",
    )(x_t, dy_t, dt_t, cum, rate, skip, s0, dse, sp, b, c, du, ry, dbl, dcl)

def sum_kernel(dal_ref, dsk_ref, out_ref, v1, v2, v3, send, recv):
    core, chip, z, partner, chips, planes, at_chip, at_z = neighbours()
    greet(partner, chips, planes, at_chip, at_z)
    v1[core] = cat0(jnp.transpose(dal_ref[...])[:OWN, :], jnp.transpose(dsk_ref[...])[:OWN, :])
    met(chips, planes)

    def copy(buf, stage, to, slot, dev):
        return rcopy(buf.at[slot], buf.at[slot], send.at[stage, to], recv.at[stage, slot], dev)

    def exchange(buf, stage, me, others, at):
        each([copy(buf, stage, o, me, at(o)) for o in others], "start")
        each([copy(buf, stage, o, o, at(o)) for o in others], "wait_recv")
        each([copy(buf, stage, o, me, at(o)) for o in others], "wait_send")

    exchange(v1, 0, core, [1 - core], lambda o: partner)
    v2[chip] = v1[0] + v1[1]
    exchange(v2, 1, chip, chips, at_chip)
    v3[z] = sum(v2[c] for c in ALL_CHIPS)
    exchange(v3, 2, z, planes, at_z)
    out_ref[...] = sum(v3[p] for p in range(PLANES))


def sum_devices(dal, dsk):
    vm = pl.BlockSpec(memory_space=pltpu.VMEM)
    V = pltpu.VMEM
    out = pl.pallas_call(
        sum_kernel,
        in_specs=[vm, vm],
        out_specs=vm,
        out_shape=jax.ShapeDtypeStruct((2 * OWN, HEADS), F32),
        scratch_shapes=[V((2, 2 * OWN, HEADS), F32), V((CHIPS, 2 * OWN, HEADS), F32), V((PLANES, 2 * OWN, HEADS), F32),
                        pltpu.SemaphoreType.DMA((3, CHIPS)), pltpu.SemaphoreType.DMA((3, CHIPS))],
        compiler_params=pltpu.CompilerParams(collective_id=1, has_side_effects=True),
        name="sum_devices",
    )(dal, dsk)
    return out[0], out[OWN]


def solution(mesh):
    tok4 = P(None, AXIS, None, None)
    tok3 = P(None, AXIS, None)

    def device_step(x_loc, dt_loc, a_log, b_loc, c_loc, d_skip, s_init, dy_loc, ds_last):
        seq = x_loc.shape[1]
        x_t = x_loc[0].transpose(1, 2, 0).reshape(HEADS * HD, seq)
        dy_t = dy_loc[0].transpose(1, 2, 0).reshape(HEADS * HD, seq)
        dt_t = dt_loc[0].T
        rate = jnp.broadcast_to((-jnp.exp(a_log) * LOG2E)[:, None], (HEADS, T))
        skip = jnp.broadcast_to(d_skip[:, None], (HEADS, T))
        b, c = b_loc[0], c_loc[0]
        flat = (HEADS * HD, N)
        du, ry, dbl, dcl, cum, start, end, first, sp = local_grads(x_t, dy_t, dt_t, rate, b, c, s_init[0], ds_last[0])
        dx, ddt, dal, dsk, db, dc = join_grads(x_t, dy_t, dt_t, cum, rate, skip, start.reshape(flat), end.reshape(flat),
                                               sp.reshape(flat), b, c, du, ry, dbl, dcl)
        grad_x = dx.reshape(HEADS, HD, seq).transpose(2, 0, 1)[None]
        grad_alog, grad_skip = sum_devices(dal, dsk)
        return grad_x, ddt.T[None], db[None], dc[None], first[None], grad_alog, grad_skip

    return jax.shard_map(device_step, mesh=mesh,
                         in_specs=(tok4, tok3, P(), tok3, tok3, P(), P(), tok4, P()),
                         out_specs=(tok4, tok3, tok3, tok3, P(), P(), P()),
                         check_vma=False)
```

```python
import functools
import jax
import jax.numpy as jnp
from jax import lax
from jax.sharding import PartitionSpec as P
from jax.experimental import pallas as pl
from jax.experimental.pallas import tpu as pltpu

AXIS = 'cp'
HEADS, HD, N = 64, 64, 128
GH = 8
GR = GH * HD
T = 128
PIECE, SHARE, OWN, CHIPS, PLANES, QS = 32, 16, 4, 4, 4, 2
ALL_CHIPS = range(CHIPS)
LOG2E = 1.4426950408889634
F32, BF16 = jnp.float32, jnp.bfloat16
MESH = pl.DeviceIdType.MESH


def mm(a, b):
    return lax.dot_general(a, b, (((1,), (0,)), ((), ())), preferred_element_type=F32)


def mm_nt(a, b):
    return lax.dot_general(a, b, (((1,), (1,)), ((), ())), preferred_element_type=F32)


def mm_tn(a, b):
    return lax.dot_general(a, b, (((0,), (0,)), ((), ())), preferred_element_type=F32)


def cat0(*parts):
    return jnp.concatenate(parts, axis=0)


def cat1(*parts):
    return jnp.concatenate(parts, axis=1)


def sum0(v):
    return jnp.sum(v, axis=0, keepdims=True)


def sum1(v):
    return jnp.sum(v, axis=1, keepdims=True)


def blk(i, size):
    return slice(i * size, (i + 1) * size)


def row(v, j):
    return v[blk(j, 1), :]


def last_col(v):
    return v[:, T - 1:T]


def split2(v):
    hi = v.astype(BF16)
    return hi, (v - hi.astype(F32)).astype(BF16)


def split3(v):
    hi = v.astype(BF16)
    r = v - hi.astype(F32)
    mid = r.astype(BF16)
    return hi, mid, (r - mid.astype(F32)).astype(BF16)


def dot_tri(v, tri):
    hi, mid, lo = split3(v)
    return mm(hi, tri) + mm(mid, tri) + mm(lo, tri)


def columns(ref, v):
    ref[...] = jnp.transpose(jnp.broadcast_to(v, (T, HEADS)))


def group(ref, g):
    return ref[pl.ds(pl.multiple_of(g * GH, GH), GH), :]


def tri_mask(upper):
    r = lax.broadcasted_iota(jnp.int32, (T, T), 0)
    c = lax.broadcasted_iota(jnp.int32, (T, T), 1)
    keep = (r <= c) if upper else (r >= c)
    return jnp.where(keep, 1.0, 0.0)


def neighbours():
    me = lax.axis_index(AXIS)
    core = lax.rem(me, 2)
    chip = lax.rem(me // 2, CHIPS)
    z = me // (2 * CHIPS)
    partner = me + 1 - 2 * core
    chips = [lax.rem(chip + r, CHIPS) for r in (2, 1, 3)]
    planes = [lax.rem(z + r, PLANES) for r in (1, 2, 3)]

    def at_chip(c):
        return me + 2 * (c - chip)

    def at_z(zz):
        return me + 2 * CHIPS * (zz - z)

    return core, chip, z, partner, chips, planes, at_chip, at_z


def greet(partner, chips, planes, at_chip, at_z):
    barrier = pltpu.get_barrier_semaphore()
    for p in [partner] + [at_chip(c) for c in chips] + [at_z(zz) for zz in planes]:
        pl.semaphore_signal(barrier, inc=1, device_id=(p,), device_id_type=MESH)


def met(chips, planes):
    pl.semaphore_wait(pltpu.get_barrier_semaphore(), 1 + len(chips) + len(planes))


def rcopy(src, dst, ssem, rsem, dev):
    return pltpu.make_async_remote_copy(src_ref=src, dst_ref=dst, send_sem=ssem, recv_sem=rsem,
                                        device_id=(dev,), device_id_type=MESH)


def each(copies, act):
    for cp in copies:
        getattr(cp, act)()


def link_steps(ng, sp, dsp, ld, s_init, ds_last, start, end, first, sp_out,
               r_s, r_ds, r_ld, c_s, c_ds, c_ld, p_s, p_ds, p_ld, t_s, t_ds, t_ld, z_b, z_ld,
               b_s, b_ds, a_s, a_ds, n_s, n_ds, o_s, o_ds, f_own, f_all,
               send0, recv0, send1, recv1, send2, recv2, send3, recv3, send4, recv4, send5, recv5, loc):
    core, chip, z, partner, chips, planes, at_chip, at_z = neighbours()
    mine, theirs = core * SHARE, (1 - core) * SHARE

    def hello():
        greet(partner, chips, planes, at_chip, at_z)

    def own_loads(q):
        part = pl.ds(q * PIECE + mine + chip * OWN, OWN)
        return [pltpu.make_async_copy(s_init.at[part], b_s.at[q, 0], loc.at[q, 0]),
                pltpu.make_async_copy(ds_last.at[part], b_ds.at[q, CHIPS - 1], loc.at[q, 1])]

    def copies0(q):
        part = pl.ds(q * PIECE + theirs, SHARE)
        logs = pl.ds(q * PIECE, PIECE)
        return [rcopy(sp.at[part], r_s.at[q], send0.at[q, 0], recv0.at[q, 0], partner),
                rcopy(dsp.at[part], r_ds.at[q], send0.at[q, 1], recv0.at[q, 1], partner),
                rcopy(ld.at[logs], r_ld.at[q], send0.at[q, 2], recv0.at[q, 2], partner)]

    def swap(q):
        if q == 0:
            met(chips, planes)
        each(copies0(q) + own_loads(q), "start")

    def copies1(q, c_dst, c_slot):
        part = pl.ds(c_dst * OWN, OWN)
        dev = at_chip(c_dst)
        return [rcopy(c_ld.at[q], p_ld.at[q, c_slot], send1.at[q, 2, c_dst], recv1.at[q, 2, c_slot], dev),
                rcopy(c_s.at[q, part], p_s.at[q, c_slot], send1.at[q, 0, c_dst], recv1.at[q, 0, c_slot], dev),
                rcopy(c_ds.at[q, part], p_ds.at[q, c_slot], send1.at[q, 1, c_dst], recv1.at[q, 1, c_slot], dev)]

    def decay(ref, q, h):
        return jnp.exp2(ref[q, pl.ds(h, 1), :])

    def pairs(q):
        each(copies0(q), "wait")
        c_ld[q] = ld[blk(q, PIECE), :] + r_ld[q]

        @pl.loop(0, SHARE)
        def _(h):
            hh = q * PIECE + mine + h
            own = jnp.exp2(ld[pl.ds(hh, 1), :])
            oth = decay(r_ld, q, mine + h)

            @pl.when(core == 0)
            def _():
                c_s[q, h] = sp[hh] * oth + r_s[q, h]
                c_ds[q, h] = dsp[hh] + own * r_ds[q, h]

            @pl.when(core == 1)
            def _():
                c_s[q, h] = r_s[q, h] * own + sp[hh]
                c_ds[q, h] = r_ds[q, h] + oth * dsp[hh]

        for c in chips:
            each(copies1(q, c, chip), "start")
        p_ld[q, chip] = c_ld[q]

        @pl.loop(0, OWN)
        def _(h):
            p_s[q, chip, h] = c_s[q, chip * OWN + h]
            p_ds[q, chip, h] = c_ds[q, chip * OWN + h]

    def copy2(q, kind, z_dst, z_slot):
        return rcopy((t_s, t_ds)[kind].at[q], z_b.at[q, z_slot], send2.at[q, 0, z_dst], recv2.at[q, 0, z_slot], at_z(z_dst))

    def copy2_ld(q, z_dst, z_slot):
        return rcopy(t_ld.at[q], z_ld.at[q, z_slot], send2.at[q, 1, z_dst], recv2.at[q, 1, z_slot], at_z(z_dst))

    def chip_decays(q, h):
        return [jnp.exp2(p_ld[q, c, pl.ds(mine + chip * OWN + h, 1), :]) for c in ALL_CHIPS]

    def z_decay(q, zz, h):
        return jnp.exp2(z_ld[q, zz, pl.ds(mine + chip * OWN + h, 1), :])

    def plane(q):
        for c in chips:
            each(copies1(q, c, c), "wait_recv")
        t_ld[q] = sum(p_ld[q, c] for c in ALL_CHIPS)

        @pl.loop(0, OWN)
        def _(h):
            d = chip_decays(q, h)
            acc = p_s[q, 0, h]
            for c in ALL_CHIPS[1:]:
                acc = acc * d[c] + p_s[q, c, h]
            t_s[q, h] = acc
            acc = p_ds[q, CHIPS - 1, h]
            for c in ALL_CHIPS[-2::-1]:
                acc = acc * d[c] + p_ds[q, c, h]
            t_ds[q, h] = acc

        for zz in planes:
            copy2_ld(q, zz, z).start()

            @pl.when(zz > z)
            def _():
                copy2(q, 0, zz, z).start()

            @pl.when(zz < z)
            def _():
                copy2(q, 1, zz, z).start()

    def copies3(q, c_dst, c_slot):
        dev = at_chip(c_dst)
        part = pl.ds(c_slot * OWN, OWN)
        return [rcopy(b_s.at[q, c_dst], a_s.at[q, part], send3.at[q, 0, c_dst], recv3.at[q, 0, c_slot], dev),
                rcopy(b_ds.at[q, c_dst], a_ds.at[q, part], send3.at[q, 1, c_dst], recv3.at[q, 1, c_slot], dev)]

    def copy_f(q, zz):
        return rcopy(f_own.at[q], f_all.at[q, pl.ds(chip * OWN, OWN)], send5.at[q, 0, zz], recv5.at[q, 0, chip], at_z(zz))

    def prefix(q):
        for zz in planes:
            copy2_ld(q, zz, zz).wait_recv()
            copy2(q, 0, zz, zz).wait_recv()
        each(own_loads(q), "wait")

        @pl.loop(0, OWN)
        def _(h):
            for zz in range(PLANES - 1):
                @pl.when(zz < z)
                def _():
                    b_s[q, 0, h] = b_s[q, 0, h] * z_decay(q, zz, h) + z_b[q, zz, h]
            for zz in range(PLANES)[:0:-1]:
                @pl.when(zz > z)
                def _():
                    b_ds[q, CHIPS - 1, h] = b_ds[q, CHIPS - 1, h] * z_decay(q, zz, h) + z_b[q, zz, h]
            d = chip_decays(q, h)
            acc = b_s[q, 0, h]
            for c in ALL_CHIPS[:-1]:
                acc = acc * d[c] + p_s[q, c, h]
                b_s[q, c + 1, h] = acc
            acc = b_ds[q, CHIPS - 1, h]
            for c in ALL_CHIPS[:0:-1]:
                acc = acc * d[c] + p_ds[q, c, h]
                b_ds[q, c - 1, h] = acc
            f_own[q, h] = acc * d[0] + p_ds[q, 0, h]
            a_s[q, chip * OWN + h] = b_s[q, chip, h]
            a_ds[q, chip * OWN + h] = b_ds[q, chip, h]

        for c in chips:
            each(copies3(q, c, chip), "start")

    def send_first():
        @pl.when(z == 0)
        def _():
            for q in range(QS):
                for zz in range(1, PLANES):
                    copy_f(q, zz).start()

                @pl.loop(0, OWN)
                def _(h):
                    f_all[q, chip * OWN + h] = f_own[q, h]

    def out_copies(q):
        part = pl.ds(q * PIECE + mine, SHARE)
        return [rcopy(o_s.at[q], start.at[part], send4.at[q, 0], recv4.at[q, 0], partner),
                rcopy(o_ds.at[q], end.at[part], send4.at[q, 1], recv4.at[q, 1], partner),
                pltpu.make_async_copy(n_s.at[q], start.at[part], loc.at[q, 2]),
                pltpu.make_async_copy(n_ds.at[q], end.at[part], loc.at[q, 3])]

    def halve(q):
        for c in chips:
            each(copies3(q, c, c), "wait_recv")

        @pl.loop(0, SHARE)
        def _(h):
            hh = q * PIECE + mine + h
            own = jnp.exp2(ld[pl.ds(hh, 1), :])
            oth = decay(r_ld, q, mine + h)

            @pl.when(core == 0)
            def _():
                n_s[q, h] = a_s[q, h]
                n_ds[q, h] = r_ds[q, h] + oth * a_ds[q, h]
                o_s[q, h] = own * a_s[q, h] + sp[hh]
                o_ds[q, h] = a_ds[q, h]

            @pl.when(core == 1)
            def _():
                n_s[q, h] = oth * a_s[q, h] + r_s[q, h]
                n_ds[q, h] = a_ds[q, h]
                o_s[q, h] = a_s[q, h]
                o_ds[q, h] = dsp[hh] + own * a_ds[q, h]

        each(out_copies(q), "start")

    def copy5(q, c_dst, c_slot):
        part = f_all.at[q, pl.ds(c_slot * OWN, OWN)]
        return rcopy(part, part, send5.at[q, 1, c_dst], recv5.at[q, 1, c_slot], at_chip(c_dst))

    def spread(q):
        @pl.when(z > 0)
        def _():
            copy_f(q, z).wait_recv()

        for c in chips:
            copy5(q, c, chip).start()

    def last(q):
        part = first.at[pl.ds(q * PIECE + mine, SHARE)]
        return [rcopy(f_all.at[q], part, send4.at[q, 2], recv4.at[q, 2], partner),
                pltpu.make_async_copy(f_all.at[q], part, loc.at[q, 4])]

    def sp_copy():
        return [pltpu.make_async_copy(sp, sp_out, loc.at[0, 5])]

    def finish():
        for q in range(QS):
            for c in chips:
                copy5(q, c, c).wait_recv()
            each(last(q), "start")
        for q in range(QS):
            each(out_copies(q), "wait")
            for c in chips:
                each(copies1(q, c, chip) + copies3(q, c, chip) + [copy5(q, c, chip)], "wait_send")
            for zz in planes:
                copy2(q, 0, zz, z).wait_send()
                copy2_ld(q, zz, z).wait_send()

            @pl.when(z == 0)
            def _():
                for zz in range(1, PLANES):
                    copy_f(q, zz).wait_send()
        each(sp_copy(), "wait")
        for q in range(QS):
            each(last(q), "wait")

    early = {0: [hello], 4: [functools.partial(swap, 0)], 6: [functools.partial(pairs, 0)],
             8: [functools.partial(swap, 1), lambda: each(sp_copy(), "start")]}
    late = [(0, 2, functools.partial(pairs, 1)), (1, 2, functools.partial(plane, 0)), (2, 5, functools.partial(plane, 1)),
            (3, 0, functools.partial(prefix, 0)), (4, 3, functools.partial(prefix, 1)), (4, 3, send_first),
            (5, 0, functools.partial(halve, 0)), (6, 2, functools.partial(halve, 1)), (6, 3, functools.partial(spread, 0)),
            (6, 5, functools.partial(spread, 1)), (7, 5, finish)]
    return early, late


def link_shapes():
    st = (HD, N)
    V = pltpu.VMEM
    D = pltpu.SemaphoreType.DMA

    def states(*lead):
        return V((QS,) + lead + st, F32)

    def logs(*lead):
        return V((QS,) + lead + (PIECE, N), F32)

    share, four, own = states(SHARE), states(CHIPS, OWN), states(OWN)
    three = D((QS, 3, CHIPS))
    two = D((QS, 2, CHIPS))
    return [share, share, logs(), share, share, logs(), four, four, logs(CHIPS), own, own, logs(), four, logs(PLANES),
            four, four, share, share, share, share, share, share, own, share,
            D((QS, 3)), D((QS, 3)), three, three, two, two, two, two, D((QS, 3)), D((QS, 3)), two, two, D((QS, 6))]


def local_kernel(nb, ng, x_ref, dy_ref, dt_ref, alog_ref, b_ref, c_ref, s_init, ds_last,
                 du_ref, ry_ref, db_ref, dc_ref, cum_out, start, end, first, sp_out,
                 gram, dgram, s_cur, ds_cur, xw, yw, y_in, u_in, rcol, cums, rates, sp, dsp, ld, *link_scratch):
    step_id = pl.program_id(0)
    early, late = link_steps(ng, sp, dsp, ld, s_init, ds_last, start, end, first, sp_out, *link_scratch)
    for at, steps in early.items():
        @pl.when(step_id == at)
        def _():
            for step in steps:
                step()

    @pl.when(step_id == 0)
    def _():
        columns(rates, -jnp.exp(alog_ref[...]) * LOG2E)

    @pl.when(step_id < ng)
    def _():
        range_states(nb, step_id, x_ref, dy_ref, dt_ref, group(rates, step_id), b_ref, c_ref, cum_out, cums, sp, dsp, ld, xw, yw)

    @pl.when(step_id >= ng)
    def _():
        local_group(nb, ng, step_id - ng, late, x_ref, dy_ref, dt_ref, b_ref, c_ref, du_ref, ry_ref, db_ref, dc_ref,
                    gram, dgram, s_cur, ds_cur, xw, yw, y_in, u_in, rcol, cums.at[step_id - ng])


def range_states(nb, g, x_ref, dy_ref, dt_ref, rate, b_ref, c_ref, cum_out, cums, sp, dsp, ld, xw, yw):
    tri = tri_mask(True).astype(BF16)
    dt = dt_ref[...]
    a = dt * rate[:, :1]
    cum, before = [], [jnp.zeros((GH, 1), F32)]
    for i in range(nb):
        v = dot_tri(a[:, blk(i, T)], tri)
        cums[g, :, blk(i, T)] = v
        cum_out[:, blk(i, T)] = v
        cum.append(v)
        before.append(before[-1] + last_col(v))
    ld[pl.ds(pl.multiple_of(g * GH, GH), GH), :] = jnp.broadcast_to(before[nb], (GH, T))
    after = jnp.zeros((GH, 1), F32)
    acc_s = jnp.zeros((GR, N), F32)
    acc_ds = jnp.zeros((GR, N), F32)
    for i in reversed(range(nb)):
        tok = blk(i, T)
        w_in = dt[:, tok] * jnp.exp2((last_col(cum[i]) - cum[i]) + after)
        w_out = jnp.exp2(cum[i] + before[i])
        after = after + last_col(cum[i])
        for j in range(GH):
            rows = blk(j, HD)
            xw[i, rows, :T], xw[i, rows, T:] = split2(x_ref[rows, tok].astype(F32) * row(w_in, j))
            yw[i, rows, :T], yw[i, rows, T:] = split2(dy_ref[rows, tok].astype(F32) * row(w_out, j))
        acc_s += mm(xw[i], cat0(b_ref[tok, :], b_ref[tok, :]))
        acc_ds += mm(yw[i], cat0(c_ref[tok, :], c_ref[tok, :]))
    for j in range(GH):
        sp[g * GH + j] = acc_s[blk(j, HD), :]
        dsp[g * GH + j] = acc_ds[blk(j, HD), :]


def local_group(nb, ng, g, late, x_ref, dy_ref, dt_ref, b_ref, c_ref, du_ref, ry_ref, db_ref, dc_ref,
                gram, dgram, s_cur, ds_cur, xw, yw, y_in, u_in, rcol, cum_ref):
    @pl.when(g == 0)
    def _():
        low = tri_mask(False)
        for i in range(nb):
            tok = blk(i, T)
            gram[i] = mm_nt(c_ref[tok, :], b_ref[tok, :]) * low
            dgram[i] = jnp.zeros((T, T), F32)
        db_ref[...] = jnp.zeros_like(db_ref)
        dc_ref[...] = jnp.zeros_like(dc_ref)
        rcol[...] = jnp.zeros_like(rcol)

    ds_cur[...] = jnp.zeros_like(ds_cur)
    s_cur[...] = jnp.zeros_like(s_cur)

    @pl.loop(0, nb)
    def _(i):
        tok = pl.ds(pl.multiple_of(i * T, T), T)
        cum = cum_ref[:, tok]
        w_in = dt_ref[:, tok] * jnp.exp2(last_col(cum) - cum)
        e_out = jnp.exp2(cum)
        for j in range(GH):
            rows = blk(j, HD)
            hi, lo = split2(x_ref[rows, tok].astype(F32) * row(w_in, j))
            xw[i, rows, :T] = hi
            xw[i, rows, T:] = lo
            hi, lo = split2(dy_ref[rows, tok].astype(F32) * row(e_out, j))
            yw[i, rows, :T] = hi
            yw[i, rows, T:] = lo
            du_ref[rows, tok] = jnp.zeros((HD, T), F32)

    @pl.loop(0, nb)
    def _(i):
        for at_g, at_i, step in late:
            @pl.when((g == at_g) & (i == at_i))
            def _():
                step()

        k = nb - 1 - i
        tok_k = pl.ds(pl.multiple_of(k * T, T), T)
        tok = pl.ds(pl.multiple_of(i * T, T), T)

        cum_k = cum_ref[:, tok_k]
        tot_k = last_col(cum_k)
        ds_hi, ds_lo = split2(ds_cur[...])
        b_k = b_ref[tok_k, :]
        c_k = c_ref[tok_k, :]
        u_in[...] = mm_nt(cat1(ds_hi, ds_lo), cat1(b_k, b_k))
        db2 = mm_tn(xw[k, :, :T], cat1(ds_hi, ds_lo))
        db_ref[tok_k, :] += db2[:, :N] + db2[:, N:] + mm_tn(xw[k, :, T:], ds_hi)
        upd_k = mm(yw[k], cat0(c_k, c_k))
        e_in = jnp.exp2(tot_k - cum_k)
        e_tot_k = jnp.exp2(tot_k)
        for j in range(GH):
            rows = blk(j, HD)
            du_ref[rows, tok_k] += u_in[rows, :] * row(e_in, j)
            ds_cur[rows, :] = ds_cur[rows, :] * row(e_tot_k, j) + upd_k[rows, :]

        cum = cum_ref[:, tok]
        e_tot = jnp.exp2(last_col(cum))
        e_out = jnp.exp2(cum)
        dt = dt_ref[:, tok]
        s_hi, s_lo = split2(s_cur[...])
        b_i = b_ref[tok, :]
        c_i = c_ref[tok, :]
        y_in[...] = mm_nt(cat1(s_hi, s_lo), cat1(c_i, c_i))
        dc2 = mm_tn(yw[i, :, :T], cat1(s_hi, s_lo))
        dc_ref[tok, :] += dc2[:, :N] + dc2[:, N:] + mm_tn(yw[i, :, T:], s_hi)
        upd = mm(xw[i], cat0(b_i, b_i))
        for j in range(GH):
            rows = blk(j, HD)
            s_cur[rows, :] = s_cur[rows, :] * row(e_tot, j) + upd[rows, :]
        cum_c = jnp.transpose(cum)
        g_i = gram[i]
        zero = jnp.zeros((HD, T), BF16)
        inter = []
        for j0 in range(0, GH, 2):
            y_t = jnp.transpose(dy_ref[pl.ds(j0 * HD, T), tok])
            u0, v0 = split2(x_ref[blk(j0, HD), tok].astype(F32) * row(dt, j0))
            u1, v1 = split2(x_ref[blk(j0 + 1, HD), tok].astype(F32) * row(dt, j0 + 1))
            pair = mm(cat1(y_t, y_t), cat1(cat0(u0, zero, v0, zero), cat0(zero, u1, zero, v1)))
            e_sum = None
            for j, p in ((j0, pair[:, :T]), (j0 + 1, pair[:, T:])):
                rows = blk(j, HD)
                lam = jnp.exp2(jnp.minimum(cum_c[:, blk(j, 1)] - row(cum, j), 0.0))
                e_sum = lam * p if e_sum is None else e_sum + lam * p
                m = lam * g_i
                rcol[:, blk(j, 1)] = sum1(m * p)
                m_hi, m_lo = split2(m)
                yb = dy_ref[rows, tok]
                du_ref[rows, tok] += mm(cat1(yb, yb), cat0(m_hi, m_lo))
                inter.append(sum0(yb.astype(F32) * y_in[rows, :]))
            dgram[i] += e_sum
        ry_ref[:, tok] = jnp.transpose(rcol[...])[:GH, :] + e_out * cat0(*inter)

    @pl.when(g == ng - 1)
    def _():
        low_f = tri_mask(False)
        for i in range(nb):
            tok = blk(i, T)
            bb = b_ref[tok, :]
            cc = c_ref[tok, :]
            hi, lo = split2(dgram[i] * low_f)
            dc_ref[tok, :] += mm(hi, bb) + mm(lo, bb)
            db_ref[tok, :] += mm_tn(hi, cc) + mm_tn(lo, cc)


def local_grads(x_t, dy_t, dt_t, a_log, b, c, s_init, ds_last):
    rows, seq = x_t.shape
    nb, ng = seq // T, rows // GR
    big = pl.BlockSpec((GR, seq), lambda g: (lax.rem(g, ng), 0))
    head = pl.BlockSpec((GH, seq), lambda g: (lax.rem(g, ng), 0))
    per_head = pl.BlockSpec((1, HEADS), lambda g: (0, 0))
    big_o = pl.BlockSpec((GR, seq), lambda g: (jnp.maximum(g - ng, 0), 0))
    head_o = pl.BlockSpec((GH, seq), lambda g: (jnp.maximum(g - ng, 0), 0))
    cum_o = pl.BlockSpec((GH, seq), lambda g: (jnp.minimum(g, ng - 1), 0))
    full = pl.BlockSpec((seq, N), lambda g: (0, 0))
    anyw = pl.BlockSpec(memory_space=pl.ANY)
    sd = jax.ShapeDtypeStruct
    state = sd((HEADS, HD, N), F32)
    V = pltpu.VMEM
    sq, grp, wide = V((nb, T, T), F32), V((GR, N), F32), V((nb, GR, 2 * T), BF16)
    return pl.pallas_call(
        functools.partial(local_kernel, nb, ng),
        grid=(2 * ng,),
        in_specs=[big, big, head, per_head, full, full, anyw, anyw],
        out_specs=[big_o, head_o, full, full, cum_o, anyw, anyw, anyw, anyw],
        out_shape=[sd((rows, seq), F32), sd((rows // HD, seq), F32), sd((seq, N), F32), sd((seq, N), F32),
                   sd((rows // HD, seq), F32), state, state, state, state],
        scratch_shapes=[sq, sq, grp, grp, wide, wide, grp, grp, V((T, T), F32), V((ng, GH, seq), F32),
                        V((HEADS, T), F32),
                        V((HEADS, HD, N), F32), V((HEADS, HD, N), F32), V((HEADS, N), F32)] + link_shapes(),
        compiler_params=pltpu.CompilerParams(dimension_semantics=("arbitrary",), collective_id=0, has_side_effects=True),
        name="local_grads",
    )(x_t, dy_t, dt_t, a_log, b, c, s_init, ds_last)


T2 = 256


def join_kernel(nb, ng, x_ref, dy_ref, dt_ref, cum_ref, alog_ref, dskip_ref, s0_ref, dse_ref, sp_ref, b_ref, c_ref,
                du_ref, ry_ref, dbl_ref, dcl_ref, f_ref,
                dx_ref, ddt_ref, dal_ref, dsk_ref, db_ref, dc_ref, first_ref,
                rates, skips, db_acc, dc_acc, ein, eout, xw, yw, s2, d2, y_in, u_in, dcum, xdu, skt):
    g = pl.program_id(0)

    @pl.when(g == 0)
    def _():
        db_acc[...] = dbl_ref[...]
        dc_acc[...] = dcl_ref[...]
        columns(rates, -jnp.exp(alog_ref[...]))
        columns(skips, dskip_ref[...])

    first_ref[...] = f_ref[...]
    rate = group(rates, g)
    skip = group(skips, g)[:, :1]
    cums = [cum_ref[:, i * T:(i + 1) * T] for i in range(nb)]
    tots = [last_col(v) for v in cums]
    acc = jnp.zeros_like(tots[0])
    for i in range(nb):
        eout[:, i * T:(i + 1) * T] = jnp.exp2(cums[i] + acc)
        acc = acc + tots[i]
    e_tot = jnp.exp2(acc)
    acc = jnp.zeros_like(tots[0])
    for i in reversed(range(nb)):
        ein[:, i * T:(i + 1) * T] = jnp.exp2((tots[i] - cums[i]) + acc)
        acc = acc + tots[i]

    s_hi, s_lo = split2(s0_ref[...])
    d_hi, d_lo = split2(dse_ref[...])
    s2[...] = cat1(s_hi, s_lo)
    d2[...] = cat1(d_hi, d_lo)

    for i in range(nb * T // T2):
        tok = blk(i, T2)
        bb = b_ref[tok, :]
        cc = c_ref[tok, :]
        y_in[...] = mm_nt(s2[...], cat1(cc, cc))
        u_in[...] = mm_nt(d2[...], cat1(bb, bb))
        dt = dt_ref[:, tok]
        e_in = ein[:, tok]
        e_out = eout[:, tok]
        w_in = dt * e_in
        xds, rys, sks = [], [], []
        for j in range(GH):
            rows = blk(j, HD)
            xf = x_ref[rows, tok].astype(F32)
            yf = dy_ref[rows, tok].astype(F32)
            du = du_ref[rows, tok] + row(e_in, j) * u_in[rows, :]
            dx_ref[rows, tok] = (row(dt, j) * du + row(skip, j) * yf).astype(BF16)
            xds.append(sum0(xf * du))
            rys.append(sum0(yf * y_in[rows, :]))
            sks.append(sum0(xf * yf))
            xw[rows, :T2], xw[rows, T2:] = split2(xf * row(w_in, j))
            yw[rows, :T2], yw[rows, T2:] = split2(yf * row(e_out, j))
        dc2 = mm_tn(yw[:, :T2], s2[...])
        dc_acc[tok, :] += dc2[:, :N] + dc2[:, N:] + mm_tn(yw[:, T2:], s2[:, :N])
        db2 = mm_tn(xw[:, :T2], d2[...])
        db_acc[tok, :] += db2[:, :N] + db2[:, N:] + mm_tn(xw[:, T2:], d2[:, :N])
        xd = cat0(*xds)
        xdu[:, tok] = xd
        dcum[:, tok] = ry_ref[:, tok] + e_out * cat0(*rys) - dt * xd
        skt[:, tok] = cat0(*sks)

    for j in range(GH):
        rows = blk(j, HD)
        dal_ref[j:j + 1, :] = jnp.sum(dse_ref[rows, :] * (sp_ref[rows, :] + row(e_tot, j) * s0_ref[rows, :]), axis=0, keepdims=True)
    run = jnp.sum(dal_ref[...], axis=1, keepdims=True)
    low = tri_mask(False).astype(BF16)
    total = jnp.zeros((GH, T), F32)
    for i in reversed(range(nb)):
        tok = blk(i, T)
        da = dot_tri(dcum[:, tok], low) + run
        run = da[:, 0:1]
        da = da * rate
        ddt_ref[:, tok] = xdu[:, tok] + da
        total = total + dt_ref[:, tok] * da
    dal_ref[...] = jnp.broadcast_to(jnp.sum(total, axis=1, keepdims=True), (GH, T))
    dsk_ref[...] = jnp.broadcast_to(jnp.sum(skt[...], axis=1, keepdims=True), (GH, T))

    @pl.when(g == ng - 1)
    def _():
        db_ref[...] = db_acc[...].astype(BF16)
        dc_ref[...] = dc_acc[...].astype(BF16)


def join_grads(x_t, dy_t, dt_t, cum, a_log, d_skip, s0, dse, sp, b, c, du, ry, dbl, dcl, first):
    rows, seq = x_t.shape
    nb, ng = seq // T, rows // GR
    big = pl.BlockSpec((GR, seq), lambda g: (g, 0))
    head = pl.BlockSpec((GH, seq), lambda g: (g, 0))
    hd1 = pl.BlockSpec((GH, T), lambda g: (g, 0))
    per_head = pl.BlockSpec((1, HEADS), lambda g: (0, 0))
    full = pl.BlockSpec((seq, N), lambda g: (0, 0))
    st = pl.BlockSpec((GR, N), lambda g: (g, 0))
    sd = jax.ShapeDtypeStruct
    return pl.pallas_call(
        functools.partial(join_kernel, nb, ng),
        grid=(ng,),
        in_specs=[big, big, head, head, per_head, per_head, st, st, st, full, full, big, head, full, full, st],
        out_specs=[big, head, hd1, hd1, full, full, st],
        out_shape=[sd((rows, seq), BF16), sd((rows // HD, seq), F32), sd((rows // HD, T), F32),
                   sd((rows // HD, T), F32), sd((seq, N), BF16), sd((seq, N), BF16), sd((rows, N), F32)],
        scratch_shapes=[pltpu.VMEM((HEADS, T), F32), pltpu.VMEM((HEADS, T), F32),
                        pltpu.VMEM((seq, N), F32), pltpu.VMEM((seq, N), F32),
                        pltpu.VMEM((GH, seq), F32), pltpu.VMEM((GH, seq), F32),
                        pltpu.VMEM((GR, 2 * T2), BF16), pltpu.VMEM((GR, 2 * T2), BF16),
                        pltpu.VMEM((GR, 2 * N), BF16), pltpu.VMEM((GR, 2 * N), BF16),
                        pltpu.VMEM((GR, T2), F32), pltpu.VMEM((GR, T2), F32),
                        pltpu.VMEM((GH, seq), F32), pltpu.VMEM((GH, seq), F32), pltpu.VMEM((GH, seq), F32)],
        compiler_params=pltpu.CompilerParams(dimension_semantics=("arbitrary",)),
        name="join_grads",
    )(x_t, dy_t, dt_t, cum, a_log, d_skip, s0, dse, sp, b, c, du, ry, dbl, dcl, first)

def sum_kernel(dal_ref, dsk_ref, al_ref, sk_ref, v1, v2, v3, send, recv):
    core, chip, z, partner, chips, planes, at_chip, at_z = neighbours()
    greet(partner, chips, planes, at_chip, at_z)
    v1[core] = cat0(jnp.transpose(dal_ref[...])[:OWN, :], jnp.transpose(dsk_ref[...])[:OWN, :])
    met(chips, planes)

    def copy(buf, stage, to, slot, dev):
        return rcopy(buf.at[slot], buf.at[slot], send.at[stage, to], recv.at[stage, slot], dev)

    def exchange(buf, stage, me, others, at):
        each([copy(buf, stage, o, me, at(o)) for o in others], "start")
        each([copy(buf, stage, o, o, at(o)) for o in others], "wait_recv")
        each([copy(buf, stage, o, me, at(o)) for o in others], "wait_send")

    exchange(v1, 0, core, [1 - core], lambda o: partner)
    v2[chip] = v1[0] + v1[1]
    exchange(v2, 1, chip, chips, at_chip)
    v3[z] = sum(v2[c] for c in ALL_CHIPS)
    exchange(v3, 2, z, planes, at_z)
    total = sum(v3[p] for p in range(PLANES))
    al_ref[...] = row(total, 0)
    sk_ref[...] = row(total, OWN)


def sum_devices(dal, dsk):
    vm = pl.BlockSpec(memory_space=pltpu.VMEM)
    V = pltpu.VMEM
    al, sk = pl.pallas_call(
        sum_kernel,
        in_specs=[vm, vm],
        out_specs=[vm, vm],
        out_shape=[jax.ShapeDtypeStruct((1, HEADS), F32)] * 2,
        scratch_shapes=[V((2, 2 * OWN, HEADS), F32), V((CHIPS, 2 * OWN, HEADS), F32), V((PLANES, 2 * OWN, HEADS), F32),
                        pltpu.SemaphoreType.DMA((3, CHIPS)), pltpu.SemaphoreType.DMA((3, CHIPS))],
        compiler_params=pltpu.CompilerParams(collective_id=1, has_side_effects=True),
        name="sum_devices",
    )(dal, dsk)
    return al[0], sk[0]


def solution(mesh):
    tok4 = P(None, AXIS, None, None)
    tok3 = P(None, AXIS, None)

    def device_step(x_loc, dt_loc, a_log, b_loc, c_loc, d_skip, s_init, dy_loc, ds_last):
        seq = x_loc.shape[1]
        x_t = x_loc[0].transpose(1, 2, 0).reshape(HEADS * HD, seq)
        dy_t = dy_loc[0].transpose(1, 2, 0).reshape(HEADS * HD, seq)
        dt_t = dt_loc[0].T
        a_row, d_row = a_log[None], d_skip[None]
        b, c = b_loc[0], c_loc[0]
        flat = (HEADS * HD, N)
        du, ry, dbl, dcl, cum, start, end, first, sp = local_grads(x_t, dy_t, dt_t, a_row, b, c, s_init[0], ds_last[0])
        dx, ddt, dal, dsk, db, dc, ds_first = join_grads(x_t, dy_t, dt_t, cum, a_row, d_row, start.reshape(flat),
                                                         end.reshape(flat), sp.reshape(flat), b, c, du, ry, dbl, dcl,
                                                         first.reshape(flat))
        grad_x = dx.reshape(HEADS, HD, seq).transpose(2, 0, 1)[None]
        grad_alog, grad_skip = sum_devices(dal, dsk)
        return grad_x, ddt.T[None], db[None], dc[None], ds_first.reshape(HEADS, HD, N)[None], grad_alog, grad_skip

    return jax.shard_map(device_step, mesh=mesh,
                         in_specs=(tok4, tok3, P(), tok3, tok3, P(), P(), tok4, P()),
                         out_specs=(tok4, tok3, tok3, tok3, P(), P(), P()),
                         check_vma=False)
```

```python
import functools
import jax
import jax.numpy as jnp
from jax import lax
from jax.sharding import PartitionSpec as P
from jax.experimental import pallas as pl
from jax.experimental.pallas import tpu as pltpu

AXIS = 'cp'
HEADS, HD, N = 64, 64, 128
GH = 8
GR = GH * HD
T = 128
PIECE, SHARE, OWN, CHIPS, PLANES, QS = 32, 16, 4, 4, 4, 2
ALL_CHIPS = range(CHIPS)
LOG2E = 1.4426950408889634
F32, BF16 = jnp.float32, jnp.bfloat16
MESH = pl.DeviceIdType.MESH


def mm(a, b):
    return lax.dot_general(a, b, (((1,), (0,)), ((), ())), preferred_element_type=F32)


def mm_nt(a, b):
    return lax.dot_general(a, b, (((1,), (1,)), ((), ())), preferred_element_type=F32)


def mm_tn(a, b):
    return lax.dot_general(a, b, (((0,), (0,)), ((), ())), preferred_element_type=F32)


def cat0(*parts):
    return jnp.concatenate(parts, axis=0)


def cat1(*parts):
    return jnp.concatenate(parts, axis=1)


def sum0(v):
    return jnp.sum(v, axis=0, keepdims=True)


def sum1(v):
    return jnp.sum(v, axis=1, keepdims=True)


def blk(i, size):
    return slice(i * size, (i + 1) * size)


def row(v, j):
    return v[blk(j, 1), :]


def last_col(v):
    return v[:, T - 1:T]


def split2(v):
    hi = v.astype(BF16)
    return hi, (v - hi.astype(F32)).astype(BF16)


def split3(v):
    hi = v.astype(BF16)
    r = v - hi.astype(F32)
    mid = r.astype(BF16)
    return hi, mid, (r - mid.astype(F32)).astype(BF16)


def dot_tri(v, tri):
    hi, mid, lo = split3(v)
    return mm(hi, tri) + mm(mid, tri) + mm(lo, tri)


def columns(ref, v):
    ref[...] = jnp.transpose(jnp.broadcast_to(v, (T, HEADS)))


def group(ref, g):
    return ref[pl.ds(pl.multiple_of(g * GH, GH), GH), :]


def tri_mask(upper):
    r = lax.broadcasted_iota(jnp.int32, (T, T), 0)
    c = lax.broadcasted_iota(jnp.int32, (T, T), 1)
    keep = (r <= c) if upper else (r >= c)
    return jnp.where(keep, 1.0, 0.0)


def neighbours():
    me = lax.axis_index(AXIS)
    core = lax.rem(me, 2)
    chip = lax.rem(me // 2, CHIPS)
    z = me // (2 * CHIPS)
    partner = me + 1 - 2 * core
    chips = [lax.rem(chip + r, CHIPS) for r in (2, 1, 3)]
    planes = [lax.rem(z + r, PLANES) for r in (1, 2, 3)]

    def at_chip(c):
        return me + 2 * (c - chip)

    def at_z(zz):
        return me + 2 * CHIPS * (zz - z)

    return core, chip, z, partner, chips, planes, at_chip, at_z


def greet(partner, chips, planes, at_chip, at_z):
    barrier = pltpu.get_barrier_semaphore()
    for p in [partner] + [at_chip(c) for c in chips] + [at_z(zz) for zz in planes]:
        pl.semaphore_signal(barrier, inc=1, device_id=(p,), device_id_type=MESH)


def met(chips, planes):
    pl.semaphore_wait(pltpu.get_barrier_semaphore(), 1 + len(chips) + len(planes))


def rcopy(src, dst, ssem, rsem, dev):
    return pltpu.make_async_remote_copy(src_ref=src, dst_ref=dst, send_sem=ssem, recv_sem=rsem,
                                        device_id=(dev,), device_id_type=MESH)


def each(copies, act):
    for cp in copies:
        getattr(cp, act)()


def link_steps(ng, sp, dsp, ld, s_init, ds_last, start, end, first, sp_out,
               r_s, r_ds, r_ld, c_s, c_ds, c_ld, p_s, p_ds, p_ld, t_s, t_ds, t_ld, z_b, z_ld,
               b_s, b_ds, a_s, a_ds, n_s, n_ds, f_own, f_all,
               send0, recv0, send1, recv1, send2, recv2, send3, recv3, send4, recv4, send5, recv5, loc):
    core, chip, z, partner, chips, planes, at_chip, at_z = neighbours()
    mine, theirs = core * SHARE, (1 - core) * SHARE

    def hello():
        greet(partner, chips, planes, at_chip, at_z)

    def own_loads(q):
        part = pl.ds(q * PIECE + mine + chip * OWN, OWN)
        return [pltpu.make_async_copy(s_init.at[part], b_s.at[q, 0], loc.at[q, 0]),
                pltpu.make_async_copy(ds_last.at[part], b_ds.at[q, CHIPS - 1], loc.at[q, 1])]

    def copies0(q):
        part = pl.ds(q * PIECE + theirs, SHARE)
        logs = pl.ds(q * PIECE, PIECE)
        return [rcopy(sp.at[part], r_s.at[q], send0.at[q, 0], recv0.at[q, 0], partner),
                rcopy(dsp.at[part], r_ds.at[q], send0.at[q, 1], recv0.at[q, 1], partner),
                rcopy(ld.at[logs], r_ld.at[q], send0.at[q, 2], recv0.at[q, 2], partner)]

    def swap(q):
        if q == 0:
            met(chips, planes)
        each(copies0(q) + own_loads(q), "start")

    def copies1(q, c_dst, c_slot):
        part = pl.ds(c_dst * OWN, OWN)
        dev = at_chip(c_dst)
        return [rcopy(c_ld.at[q], p_ld.at[q, c_slot], send1.at[q, 2, c_dst], recv1.at[q, 2, c_slot], dev),
                rcopy(c_s.at[q, part], p_s.at[q, c_slot], send1.at[q, 0, c_dst], recv1.at[q, 0, c_slot], dev),
                rcopy(c_ds.at[q, part], p_ds.at[q, c_slot], send1.at[q, 1, c_dst], recv1.at[q, 1, c_slot], dev)]

    def decay(ref, q, h):
        return jnp.exp2(ref[q, pl.ds(h, 1), :])

    def by_core(q, lower, upper):
        for k, run in enumerate((lower, upper)):
            @pl.when(core == k)
            def _():
                for h in range(SHARE):
                    hh = q * PIECE + mine + h
                    run(h, hh, jnp.exp2(ld[pl.ds(hh, 1), :]), decay(r_ld, q, mine + h))

    def pairs(q):
        each(copies0(q), "wait")
        c_ld[q] = ld[blk(q, PIECE), :] + r_ld[q]

        def join_lower(h, hh, own, oth):
            c_s[q, h] = sp[hh] * oth + r_s[q, h]
            c_ds[q, h] = dsp[hh] + own * r_ds[q, h]

        def join_upper(h, hh, own, oth):
            c_s[q, h] = r_s[q, h] * own + sp[hh]
            c_ds[q, h] = r_ds[q, h] + oth * dsp[hh]

        by_core(q, join_lower, join_upper)
        for c in chips:
            each(copies1(q, c, chip), "start")
        p_ld[q, chip] = c_ld[q]

        for h in range(OWN):
            p_s[q, chip, h] = c_s[q, chip * OWN + h]
            p_ds[q, chip, h] = c_ds[q, chip * OWN + h]

    def copy2(q, kind, z_dst, z_slot):
        return rcopy((t_s, t_ds)[kind].at[q], z_b.at[q, z_slot], send2.at[q, 0, z_dst], recv2.at[q, 0, z_slot], at_z(z_dst))

    def copy2_ld(q, z_dst, z_slot):
        return rcopy(t_ld.at[q], z_ld.at[q, z_slot], send2.at[q, 1, z_dst], recv2.at[q, 1, z_slot], at_z(z_dst))

    def chip_decays(q, h):
        return [jnp.exp2(p_ld[q, c, pl.ds(mine + chip * OWN + h, 1), :]) for c in ALL_CHIPS]

    def z_decay(q, zz, h):
        return jnp.exp2(z_ld[q, zz, pl.ds(mine + chip * OWN + h, 1), :])

    def plane(q):
        for c in chips:
            each(copies1(q, c, c), "wait_recv")
        t_ld[q] = sum(p_ld[q, c] for c in ALL_CHIPS)

        for h in range(OWN):
            d = chip_decays(q, h)
            acc = p_s[q, 0, h]
            for c in ALL_CHIPS[1:]:
                acc = acc * d[c] + p_s[q, c, h]
            t_s[q, h] = acc
            acc = p_ds[q, CHIPS - 1, h]
            for c in ALL_CHIPS[-2::-1]:
                acc = acc * d[c] + p_ds[q, c, h]
            t_ds[q, h] = acc

        for zz in planes:
            copy2_ld(q, zz, z).start()

            @pl.when(zz > z)
            def _():
                copy2(q, 0, zz, z).start()

            @pl.when(zz < z)
            def _():
                copy2(q, 1, zz, z).start()

    def copies3(q, c_dst, c_slot):
        dev = at_chip(c_dst)
        part = pl.ds(c_slot * OWN, OWN)
        return [rcopy(b_s.at[q, c_dst], a_s.at[q, part], send3.at[q, 0, c_dst], recv3.at[q, 0, c_slot], dev),
                rcopy(b_ds.at[q, c_dst], a_ds.at[q, part], send3.at[q, 1, c_dst], recv3.at[q, 1, c_slot], dev)]

    def copy_f(q, zz):
        return rcopy(f_own.at[q], f_all.at[q, pl.ds(chip * OWN, OWN)], send5.at[q, 0, zz], recv5.at[q, 0, chip], at_z(zz))

    def prefix(q):
        for zz in planes:
            copy2_ld(q, zz, zz).wait_recv()
            copy2(q, 0, zz, zz).wait_recv()
        each(own_loads(q), "wait")

        for zz in range(PLANES - 1):
            @pl.when(zz < z)
            def _():
                for h in range(OWN):
                    b_s[q, 0, h] = b_s[q, 0, h] * z_decay(q, zz, h) + z_b[q, zz, h]
        for zz in range(PLANES)[:0:-1]:
            @pl.when(zz > z)
            def _():
                for h in range(OWN):
                    b_ds[q, CHIPS - 1, h] = b_ds[q, CHIPS - 1, h] * z_decay(q, zz, h) + z_b[q, zz, h]
        for h in range(OWN):
            d = chip_decays(q, h)
            acc = b_s[q, 0, h]
            for c in ALL_CHIPS[:-1]:
                acc = acc * d[c] + p_s[q, c, h]
                b_s[q, c + 1, h] = acc
            acc = b_ds[q, CHIPS - 1, h]
            for c in ALL_CHIPS[:0:-1]:
                acc = acc * d[c] + p_ds[q, c, h]
                b_ds[q, c - 1, h] = acc
            f_own[q, h] = acc * d[0] + p_ds[q, 0, h]
            a_s[q, chip * OWN + h] = b_s[q, chip, h]
            a_ds[q, chip * OWN + h] = b_ds[q, chip, h]

        for c in chips:
            each(copies3(q, c, chip), "start")

    def send_first():
        @pl.when(z == 0)
        def _():
            for q in range(QS):
                for zz in range(1, PLANES):
                    copy_f(q, zz).start()

                @pl.loop(0, OWN)
                def _(h):
                    f_all[q, chip * OWN + h] = f_own[q, h]

    def out_copies(q, far_s, far_ds, near_s, near_ds):
        part = pl.ds(q * PIECE + mine, SHARE)
        return [rcopy(far_s.at[q], start.at[part], send4.at[q, 0], recv4.at[q, 0], partner),
                rcopy(far_ds.at[q], end.at[part], send4.at[q, 1], recv4.at[q, 1], partner),
                pltpu.make_async_copy(near_s.at[q], start.at[part], loc.at[q, 2]),
                pltpu.make_async_copy(near_ds.at[q], end.at[part], loc.at[q, 3])]

    def halve(q):
        for c in chips:
            each(copies3(q, c, c), "wait_recv")

        def lower(h, hh, own, oth):
            n_s[q, h] = own * a_s[q, h] + sp[hh]
            n_ds[q, h] = r_ds[q, h] + oth * a_ds[q, h]

        def upper(h, hh, own, oth):
            n_s[q, h] = oth * a_s[q, h] + r_s[q, h]
            n_ds[q, h] = dsp[hh] + own * a_ds[q, h]

        by_core(q, lower, upper)

        @pl.when(core == 0)
        def _():
            each(out_copies(q, n_s, a_ds, a_s, n_ds), "start")

        @pl.when(core == 1)
        def _():
            each(out_copies(q, a_s, n_ds, n_s, a_ds), "start")

    def copy5(q, c_dst, c_slot):
        part = f_all.at[q, pl.ds(c_slot * OWN, OWN)]
        return rcopy(part, part, send5.at[q, 1, c_dst], recv5.at[q, 1, c_slot], at_chip(c_dst))

    def spread(q):
        @pl.when(z > 0)
        def _():
            copy_f(q, z).wait_recv()

        for c in chips:
            copy5(q, c, chip).start()

    def last(q):
        part = first.at[pl.ds(q * PIECE + mine, SHARE)]
        return [rcopy(f_all.at[q], part, send4.at[q, 2], recv4.at[q, 2], partner),
                pltpu.make_async_copy(f_all.at[q], part, loc.at[q, 4])]

    def sp_copy():
        return [pltpu.make_async_copy(sp, sp_out, loc.at[0, 5])]

    def finish():
        for q in range(QS):
            for c in chips:
                copy5(q, c, c).wait_recv()
            each(last(q), "start")
        for q in range(QS):
            each(out_copies(q, n_s, a_ds, a_s, n_ds), "wait")
            for c in chips:
                each(copies1(q, c, chip) + copies3(q, c, chip) + [copy5(q, c, chip)], "wait_send")
            for zz in planes:
                copy2(q, 0, zz, z).wait_send()
                copy2_ld(q, zz, z).wait_send()

            @pl.when(z == 0)
            def _():
                for zz in range(1, PLANES):
                    copy_f(q, zz).wait_send()
        each(sp_copy(), "wait")
        for q in range(QS):
            each(last(q), "wait")

    early = {0: [hello], 4: [functools.partial(swap, 0)], 6: [functools.partial(pairs, 0)],
             8: [functools.partial(swap, 1), lambda: each(sp_copy(), "start")]}
    late = [(0, 2, functools.partial(pairs, 1)), (1, 2, functools.partial(plane, 0)), (2, 5, functools.partial(plane, 1)),
            (3, 0, functools.partial(prefix, 0)), (4, 3, functools.partial(prefix, 1)), (4, 3, send_first),
            (5, 0, functools.partial(halve, 0)), (6, 2, functools.partial(halve, 1)), (6, 3, functools.partial(spread, 0)),
            (6, 5, functools.partial(spread, 1)), (7, 5, finish)]
    return early, late


def link_shapes():
    st = (HD, N)
    V = pltpu.VMEM
    D = pltpu.SemaphoreType.DMA

    def states(*lead):
        return V((QS,) + lead + st, F32)

    def logs(*lead):
        return V((QS,) + lead + (PIECE, N), F32)

    share, four, own = states(SHARE), states(CHIPS, OWN), states(OWN)
    three = D((QS, 3, CHIPS))
    two = D((QS, 2, CHIPS))
    return [share, share, logs(), share, share, logs(), four, four, logs(CHIPS), own, own, logs(), four, logs(PLANES),
            four, four, share, share, share, share, own, share,
            D((QS, 3)), D((QS, 3)), three, three, two, two, two, two, D((QS, 3)), D((QS, 3)), two, two, D((QS, 6))]


def local_kernel(nb, ng, x_ref, dy_ref, dt_ref, alog_ref, b_ref, c_ref, s_init, ds_last,
                 du_ref, ry_ref, db_ref, dc_ref, cum_out, start, end, first, sp_out,
                 gram, dgram, s_cur, ds_cur, xw, yw, y_in, u_in, rcol, cums, rates, sp, dsp, ld, *link_scratch):
    step_id = pl.program_id(0)
    early, late = link_steps(ng, sp, dsp, ld, s_init, ds_last, start, end, first, sp_out, *link_scratch)
    for at, steps in early.items():
        @pl.when(step_id == at)
        def _():
            for step in steps:
                step()

    @pl.when(step_id == 0)
    def _():
        columns(rates, -jnp.exp(alog_ref[...]) * LOG2E)

    @pl.when(step_id < ng)
    def _():
        range_states(nb, step_id, x_ref, dy_ref, dt_ref, group(rates, step_id), b_ref, c_ref, cum_out, cums, sp, dsp, ld, xw, yw)

    @pl.when(step_id >= ng)
    def _():
        local_group(nb, ng, step_id - ng, late, x_ref, dy_ref, dt_ref, b_ref, c_ref, du_ref, ry_ref, db_ref, dc_ref,
                    gram, dgram, s_cur, ds_cur, xw, yw, y_in, u_in, rcol, cums.at[step_id - ng])


def range_states(nb, g, x_ref, dy_ref, dt_ref, rate, b_ref, c_ref, cum_out, cums, sp, dsp, ld, xw, yw):
    tri = tri_mask(True).astype(BF16)
    dt = dt_ref[...]
    a = dt * rate[:, :1]
    cum, before = [], [jnp.zeros((GH, 1), F32)]
    for i in range(nb):
        v = dot_tri(a[:, blk(i, T)], tri)
        cums[g, :, blk(i, T)] = v
        cum_out[:, blk(i, T)] = v
        cum.append(v)
        before.append(before[-1] + last_col(v))
    ld[pl.ds(pl.multiple_of(g * GH, GH), GH), :] = jnp.broadcast_to(before[nb], (GH, T))
    after = jnp.zeros((GH, 1), F32)
    acc_s = jnp.zeros((GR, N), F32)
    acc_ds = jnp.zeros((GR, N), F32)
    for i in reversed(range(nb)):
        tok = blk(i, T)
        w_in = dt[:, tok] * jnp.exp2((last_col(cum[i]) - cum[i]) + after)
        w_out = jnp.exp2(cum[i] + before[i])
        after = after + last_col(cum[i])
        for j in range(GH):
            rows = blk(j, HD)
            xw[i, rows, :T], xw[i, rows, T:] = split2(x_ref[rows, tok].astype(F32) * row(w_in, j))
            yw[i, rows, :T], yw[i, rows, T:] = split2(dy_ref[rows, tok].astype(F32) * row(w_out, j))
        acc_s += mm(xw[i], cat0(b_ref[tok, :], b_ref[tok, :]))
        acc_ds += mm(yw[i], cat0(c_ref[tok, :], c_ref[tok, :]))
    for j in range(GH):
        sp[g * GH + j] = acc_s[blk(j, HD), :]
        dsp[g * GH + j] = acc_ds[blk(j, HD), :]


def carry(state, weighted, k, other, tot, first):
    upd = mm(weighted[k], cat0(other, other))
    if first:
        state[...] = upd
        return
    decay = jnp.exp2(tot)
    for j in range(GH):
        rows = blk(j, HD)
        state[rows, :] = state[rows, :] * row(decay, j) + upd[rows, :]


def local_group(nb, ng, g, late, x_ref, dy_ref, dt_ref, b_ref, c_ref, du_ref, ry_ref, db_ref, dc_ref,
                gram, dgram, s_cur, ds_cur, xw, yw, y_in, u_in, rcol, cum_ref):
    @pl.when(g == 0)
    def _():
        low = tri_mask(False)
        for i in range(nb):
            tok = blk(i, T)
            gram[i] = mm_nt(c_ref[tok, :], b_ref[tok, :]) * low
            dgram[i] = jnp.zeros((T, T), F32)
        db_ref[...] = jnp.zeros_like(db_ref)
        dc_ref[...] = jnp.zeros_like(dc_ref)
        rcol[...] = jnp.zeros_like(rcol)

    @pl.loop(0, nb)
    def _(i):
        tok = pl.ds(pl.multiple_of(i * T, T), T)
        cum = cum_ref[:, tok]
        w_in = dt_ref[:, tok] * jnp.exp2(last_col(cum) - cum)
        e_out = jnp.exp2(cum)
        for j in range(GH):
            rows = blk(j, HD)
            hi, lo = split2(x_ref[rows, tok].astype(F32) * row(w_in, j))
            xw[i, rows, :T] = hi
            xw[i, rows, T:] = lo
            hi, lo = split2(dy_ref[rows, tok].astype(F32) * row(e_out, j))
            yw[i, rows, :T] = hi
            yw[i, rows, T:] = lo
            du_ref[rows, tok] = jnp.zeros((HD, T), F32)

    def block(i, first):
        for at_g, at_i, step in late:
            if (at_i == 0) == first:
                pl.when((g == at_g) if first else (g == at_g) & (i == at_i))(step)

        k = nb - 1 - i
        tok_k, tok = (blk(k, T), blk(i, T)) if first else (pl.ds(pl.multiple_of(k * T, T), T), pl.ds(pl.multiple_of(i * T, T), T))

        cum_k = cum_ref[:, tok_k]
        tot_k = last_col(cum_k)
        b_k = b_ref[tok_k, :]
        c_k = c_ref[tok_k, :]
        if not first:
            ds_hi, ds_lo = split2(ds_cur[...])
            u_in[...] = mm_nt(cat1(ds_hi, ds_lo), cat1(b_k, b_k))
            db2 = mm_tn(xw[k, :, :T], cat1(ds_hi, ds_lo))
            db_ref[tok_k, :] += db2[:, :N] + db2[:, N:] + mm_tn(xw[k, :, T:], ds_hi)
            e_in = jnp.exp2(tot_k - cum_k)
            for j in range(GH):
                rows = blk(j, HD)
                du_ref[rows, tok_k] += u_in[rows, :] * row(e_in, j)
        carry(ds_cur, yw, k, c_k, tot_k, first)

        cum = cum_ref[:, tok]
        e_out = jnp.exp2(cum)
        dt = dt_ref[:, tok]
        b_i = b_ref[tok, :]
        c_i = c_ref[tok, :]
        if not first:
            s_hi, s_lo = split2(s_cur[...])
            y_in[...] = mm_nt(cat1(s_hi, s_lo), cat1(c_i, c_i))
            dc2 = mm_tn(yw[i, :, :T], cat1(s_hi, s_lo))
            dc_ref[tok, :] += dc2[:, :N] + dc2[:, N:] + mm_tn(yw[i, :, T:], s_hi)
        carry(s_cur, xw, i, b_i, last_col(cum), first)
        cum_c = jnp.transpose(cum)
        g_i = gram[i]
        zero = jnp.zeros((HD, T), BF16)
        inter = []
        for j0 in range(0, GH, 2):
            y_t = jnp.transpose(dy_ref[pl.ds(j0 * HD, T), tok])
            u0, v0 = split2(x_ref[blk(j0, HD), tok].astype(F32) * row(dt, j0))
            u1, v1 = split2(x_ref[blk(j0 + 1, HD), tok].astype(F32) * row(dt, j0 + 1))
            pair = mm(cat1(y_t, y_t), cat1(cat0(u0, zero, v0, zero), cat0(zero, u1, zero, v1)))
            e_sum = None
            for j, p in ((j0, pair[:, :T]), (j0 + 1, pair[:, T:])):
                rows = blk(j, HD)
                lam = jnp.exp2(jnp.minimum(cum_c[:, blk(j, 1)] - row(cum, j), 0.0))
                e_sum = lam * p if e_sum is None else e_sum + lam * p
                m = lam * g_i
                rcol[:, blk(j, 1)] = sum1(m * p)
                m_hi, m_lo = split2(m)
                yb = dy_ref[rows, tok]
                du_ref[rows, tok] += mm(cat1(yb, yb), cat0(m_hi, m_lo))
                if not first:
                    inter.append(sum0(yb.astype(F32) * y_in[rows, :]))
            dgram[i] += e_sum
        own = jnp.transpose(rcol[...])[:GH, :]
        ry_ref[:, tok] = own + e_out * cat0(*inter) if inter else own

    block(0, True)

    @pl.loop(1, nb)
    def _(i):
        block(i, False)

    @pl.when(g == ng - 1)
    def _():
        low_f = tri_mask(False)
        for i in range(nb):
            tok = blk(i, T)
            bb = b_ref[tok, :]
            cc = c_ref[tok, :]
            hi, lo = split2(dgram[i] * low_f)
            dc_ref[tok, :] += mm(hi, bb) + mm(lo, bb)
            db_ref[tok, :] += mm_tn(hi, cc) + mm_tn(lo, cc)


def local_grads(x_t, dy_t, dt_t, a_log, b, c, s_init, ds_last):
    rows, seq = x_t.shape
    nb, ng = seq // T, rows // GR
    big = pl.BlockSpec((GR, seq), lambda g: (lax.rem(g, ng), 0))
    head = pl.BlockSpec((GH, seq), lambda g: (lax.rem(g, ng), 0))
    per_head = pl.BlockSpec((1, HEADS), lambda g: (0, 0))
    big_o = pl.BlockSpec((GR, seq), lambda g: (jnp.maximum(g - ng, 0), 0))
    head_o = pl.BlockSpec((GH, seq), lambda g: (jnp.maximum(g - ng, 0), 0))
    cum_o = pl.BlockSpec((GH, seq), lambda g: (jnp.minimum(g, ng - 1), 0))
    full = pl.BlockSpec((seq, N), lambda g: (0, 0))
    anyw = pl.BlockSpec(memory_space=pl.ANY)
    sd = jax.ShapeDtypeStruct
    state = sd((HEADS, HD, N), F32)
    V = pltpu.VMEM
    sq, grp, wide = V((nb, T, T), F32), V((GR, N), F32), V((nb, GR, 2 * T), BF16)
    return pl.pallas_call(
        functools.partial(local_kernel, nb, ng),
        grid=(2 * ng,),
        in_specs=[big, big, head, per_head, full, full, anyw, anyw],
        out_specs=[big_o, head_o, full, full, cum_o, anyw, anyw, anyw, anyw],
        out_shape=[sd((rows, seq), F32), sd((rows // HD, seq), F32), sd((seq, N), F32), sd((seq, N), F32),
                   sd((rows // HD, seq), F32), state, state, state, state],
        scratch_shapes=[sq, sq, grp, grp, wide, wide, grp, grp, V((T, T), F32), V((ng, GH, seq), F32),
                        V((HEADS, T), F32),
                        V((HEADS, HD, N), F32), V((HEADS, HD, N), F32), V((HEADS, N), F32)] + link_shapes(),
        compiler_params=pltpu.CompilerParams(dimension_semantics=("arbitrary",), collective_id=0, has_side_effects=True),
        name="local_grads",
    )(x_t, dy_t, dt_t, a_log, b, c, s_init, ds_last)


T2 = 256


def join_kernel(nb, ng, x_ref, dy_ref, dt_ref, cum_ref, alog_ref, dskip_ref, s0_ref, dse_ref, sp_ref, b_ref, c_ref,
                du_ref, ry_ref, dbl_ref, dcl_ref, f_ref,
                dx_ref, ddt_ref, dal_ref, dsk_ref, db_ref, dc_ref, first_ref,
                rates, skips, db_acc, dc_acc, ein, eout, xw, yw, s2, d2, y_in, u_in, dcum, xdu, skt):
    g = pl.program_id(0)

    @pl.when(g == 0)
    def _():
        db_acc[...] = dbl_ref[...]
        dc_acc[...] = dcl_ref[...]
        columns(rates, -jnp.exp(alog_ref[...]))
        columns(skips, dskip_ref[...])

    first_ref[...] = f_ref[...]
    rate = group(rates, g)
    skip = group(skips, g)[:, :1]
    cums = [cum_ref[:, i * T:(i + 1) * T] for i in range(nb)]
    tots = [last_col(v) for v in cums]
    acc = jnp.zeros_like(tots[0])
    for i in range(nb):
        eout[:, i * T:(i + 1) * T] = jnp.exp2(cums[i] + acc)
        acc = acc + tots[i]
    e_tot = jnp.exp2(acc)
    acc = jnp.zeros_like(tots[0])
    for i in reversed(range(nb)):
        ein[:, i * T:(i + 1) * T] = jnp.exp2((tots[i] - cums[i]) + acc)
        acc = acc + tots[i]

    s_hi, s_lo = split2(s0_ref[...])
    d_hi, d_lo = split2(dse_ref[...])
    s2[...] = cat1(s_hi, s_lo)
    d2[...] = cat1(d_hi, d_lo)

    for i in range(nb * T // T2):
        tok = blk(i, T2)
        bb = b_ref[tok, :]
        cc = c_ref[tok, :]
        y_in[...] = mm_nt(s2[...], cat1(cc, cc))
        u_in[...] = mm_nt(d2[...], cat1(bb, bb))
        dt = dt_ref[:, tok]
        e_in = ein[:, tok]
        e_out = eout[:, tok]
        w_in = dt * e_in
        xds, rys, sks = [], [], []
        for j in range(GH):
            rows = blk(j, HD)
            xf = x_ref[rows, tok].astype(F32)
            yf = dy_ref[rows, tok].astype(F32)
            du = du_ref[rows, tok] + row(e_in, j) * u_in[rows, :]
            dx_ref[rows, tok] = (row(dt, j) * du + row(skip, j) * yf).astype(BF16)
            xds.append(sum0(xf * du))
            rys.append(sum0(yf * y_in[rows, :]))
            sks.append(sum0(xf * yf))
            xw[rows, :T2], xw[rows, T2:] = split2(xf * row(w_in, j))
            yw[rows, :T2], yw[rows, T2:] = split2(yf * row(e_out, j))
        dc2 = mm_tn(yw[:, :T2], s2[...])
        dc_acc[tok, :] += dc2[:, :N] + dc2[:, N:] + mm_tn(yw[:, T2:], s2[:, :N])
        db2 = mm_tn(xw[:, :T2], d2[...])
        db_acc[tok, :] += db2[:, :N] + db2[:, N:] + mm_tn(xw[:, T2:], d2[:, :N])
        xd = cat0(*xds)
        xdu[:, tok] = xd
        dcum[:, tok] = ry_ref[:, tok] + e_out * cat0(*rys) - dt * xd
        skt[:, tok] = cat0(*sks)

    for j in range(GH):
        rows = blk(j, HD)
        dal_ref[j:j + 1, :] = jnp.sum(dse_ref[rows, :] * (sp_ref[rows, :] + row(e_tot, j) * s0_ref[rows, :]), axis=0, keepdims=True)
    run = jnp.sum(dal_ref[...], axis=1, keepdims=True)
    low = tri_mask(False).astype(BF16)
    total = jnp.zeros((GH, T), F32)
    for i in reversed(range(nb)):
        tok = blk(i, T)
        da = dot_tri(dcum[:, tok], low) + run
        run = da[:, 0:1]
        da = da * rate
        ddt_ref[:, tok] = xdu[:, tok] + da
        total = total + dt_ref[:, tok] * da
    dal_ref[...] = jnp.broadcast_to(jnp.sum(total, axis=1, keepdims=True), (GH, T))
    dsk_ref[...] = jnp.broadcast_to(jnp.sum(skt[...], axis=1, keepdims=True), (GH, T))

    @pl.when(g == ng - 1)
    def _():
        db_ref[...] = db_acc[...].astype(BF16)
        dc_ref[...] = dc_acc[...].astype(BF16)


def join_grads(x_t, dy_t, dt_t, cum, a_log, d_skip, s0, dse, sp, b, c, du, ry, dbl, dcl, first):
    rows, seq = x_t.shape
    nb, ng = seq // T, rows // GR
    big = pl.BlockSpec((GR, seq), lambda g: (g, 0))
    head = pl.BlockSpec((GH, seq), lambda g: (g, 0))
    hd1 = pl.BlockSpec((GH, T), lambda g: (g, 0))
    per_head = pl.BlockSpec((1, HEADS), lambda g: (0, 0))
    full = pl.BlockSpec((seq, N), lambda g: (0, 0))
    st = pl.BlockSpec((GR, N), lambda g: (g, 0))
    sd = jax.ShapeDtypeStruct
    return pl.pallas_call(
        functools.partial(join_kernel, nb, ng),
        grid=(ng,),
        in_specs=[big, big, head, head, per_head, per_head, st, st, st, full, full, big, head, full, full, st],
        out_specs=[big, head, hd1, hd1, full, full, st],
        out_shape=[sd((rows, seq), BF16), sd((rows // HD, seq), F32), sd((rows // HD, T), F32),
                   sd((rows // HD, T), F32), sd((seq, N), BF16), sd((seq, N), BF16), sd((rows, N), F32)],
        scratch_shapes=[pltpu.VMEM((HEADS, T), F32), pltpu.VMEM((HEADS, T), F32),
                        pltpu.VMEM((seq, N), F32), pltpu.VMEM((seq, N), F32),
                        pltpu.VMEM((GH, seq), F32), pltpu.VMEM((GH, seq), F32),
                        pltpu.VMEM((GR, 2 * T2), BF16), pltpu.VMEM((GR, 2 * T2), BF16),
                        pltpu.VMEM((GR, 2 * N), BF16), pltpu.VMEM((GR, 2 * N), BF16),
                        pltpu.VMEM((GR, T2), F32), pltpu.VMEM((GR, T2), F32),
                        pltpu.VMEM((GH, seq), F32), pltpu.VMEM((GH, seq), F32), pltpu.VMEM((GH, seq), F32)],
        compiler_params=pltpu.CompilerParams(dimension_semantics=("arbitrary",)),
        name="join_grads",
    )(x_t, dy_t, dt_t, cum, a_log, d_skip, s0, dse, sp, b, c, du, ry, dbl, dcl, first)

def sum_kernel(dal_ref, dsk_ref, al_ref, sk_ref, v1, v2, v3, send, recv):
    core, chip, z, partner, chips, planes, at_chip, at_z = neighbours()
    greet(partner, chips, planes, at_chip, at_z)
    v1[core] = cat0(jnp.transpose(dal_ref[...])[:OWN, :], jnp.transpose(dsk_ref[...])[:OWN, :])
    met(chips, planes)

    def copy(buf, stage, to, slot, dev):
        return rcopy(buf.at[slot], buf.at[slot], send.at[stage, to], recv.at[stage, slot], dev)

    def exchange(buf, stage, me, others, at):
        each([copy(buf, stage, o, me, at(o)) for o in others], "start")
        each([copy(buf, stage, o, o, at(o)) for o in others], "wait_recv")
        each([copy(buf, stage, o, me, at(o)) for o in others], "wait_send")

    exchange(v1, 0, core, [1 - core], lambda o: partner)
    v2[chip] = v1[0] + v1[1]
    exchange(v2, 1, chip, chips, at_chip)
    v3[z] = sum(v2[c] for c in ALL_CHIPS)
    exchange(v3, 2, z, planes, at_z)
    total = sum(v3[p] for p in range(PLANES))
    al_ref[...] = row(total, 0)
    sk_ref[...] = row(total, OWN)


def sum_devices(dal, dsk):
    vm = pl.BlockSpec(memory_space=pltpu.VMEM)
    V = pltpu.VMEM
    al, sk = pl.pallas_call(
        sum_kernel,
        in_specs=[vm, vm],
        out_specs=[vm, vm],
        out_shape=[jax.ShapeDtypeStruct((1, HEADS), F32)] * 2,
        scratch_shapes=[V((2, 2 * OWN, HEADS), F32), V((CHIPS, 2 * OWN, HEADS), F32), V((PLANES, 2 * OWN, HEADS), F32),
                        pltpu.SemaphoreType.DMA((3, CHIPS)), pltpu.SemaphoreType.DMA((3, CHIPS))],
        compiler_params=pltpu.CompilerParams(collective_id=1, has_side_effects=True),
        name="sum_devices",
    )(dal, dsk)
    return al[0], sk[0]


def solution(mesh):
    tok4 = P(None, AXIS, None, None)
    tok3 = P(None, AXIS, None)

    def device_step(x_loc, dt_loc, a_log, b_loc, c_loc, d_skip, s_init, dy_loc, ds_last):
        seq = x_loc.shape[1]
        x_t = x_loc[0].transpose(1, 2, 0).reshape(HEADS * HD, seq)
        dy_t = dy_loc[0].transpose(1, 2, 0).reshape(HEADS * HD, seq)
        dt_t = dt_loc[0].T
        a_row, d_row = a_log[None], d_skip[None]
        b, c = b_loc[0], c_loc[0]
        flat = (HEADS * HD, N)
        du, ry, dbl, dcl, cum, start, end, first, sp = local_grads(x_t, dy_t, dt_t, a_row, b, c, s_init[0], ds_last[0])
        dx, ddt, dal, dsk, db, dc, ds_first = join_grads(x_t, dy_t, dt_t, cum, a_row, d_row, start.reshape(flat),
                                                         end.reshape(flat), sp.reshape(flat), b, c, du, ry, dbl, dcl,
                                                         first.reshape(flat))
        grad_x = dx.reshape(HEADS, HD, seq).transpose(2, 0, 1)[None]
        grad_alog, grad_skip = sum_devices(dal, dsk)
        return grad_x, ddt.T[None], db[None], dc[None], ds_first.reshape(HEADS, HD, N)[None], grad_alog, grad_skip

    return jax.shard_map(device_step, mesh=mesh,
                         in_specs=(tok4, tok3, P(), tok3, tok3, P(), P(), tok4, P()),
                         out_specs=(tok4, tok3, tok3, tok3, P(), P(), P()),
                         check_vma=False)
```

```python
import functools
import jax
import jax.numpy as jnp
from jax import lax
from jax.sharding import PartitionSpec as P
from jax.experimental import pallas as pl
from jax.experimental.pallas import tpu as pltpu

AXIS = 'cp'
HEADS, HD, N = 64, 64, 128
GH = 8
GR = GH * HD
T = 128
PIECE, SHARE, OWN, CHIPS, PLANES, QS = 32, 16, 4, 4, 4, 2
ALL_CHIPS = range(CHIPS)
LOG2E = 1.4426950408889634
F32, BF16 = jnp.float32, jnp.bfloat16
MESH = pl.DeviceIdType.MESH


def mm(a, b):
    return lax.dot_general(a, b, (((1,), (0,)), ((), ())), preferred_element_type=F32)


def mm_nt(a, b):
    return lax.dot_general(a, b, (((1,), (1,)), ((), ())), preferred_element_type=F32)


def mm_tn(a, b):
    return lax.dot_general(a, b, (((0,), (0,)), ((), ())), preferred_element_type=F32)


def cat0(*parts):
    return jnp.concatenate(parts, axis=0)


def cat1(*parts):
    return jnp.concatenate(parts, axis=1)


def sum0(v):
    return jnp.sum(v, axis=0, keepdims=True)


def sum1(v):
    return jnp.sum(v, axis=1, keepdims=True)


def blk(i, size):
    return slice(i * size, (i + 1) * size)


def row(v, j):
    return v[blk(j, 1), :]


def last_col(v):
    return v[:, T - 1:T]


def split2(v):
    hi = v.astype(BF16)
    return hi, (v - hi.astype(F32)).astype(BF16)


def split3(v):
    hi = v.astype(BF16)
    r = v - hi.astype(F32)
    mid = r.astype(BF16)
    return hi, mid, (r - mid.astype(F32)).astype(BF16)


def dot_tri(v, tri):
    hi, mid, lo = split3(v)
    return mm(hi, tri) + mm(mid, tri) + mm(lo, tri)


def columns(ref, v):
    ref[...] = jnp.transpose(jnp.broadcast_to(v, (T, HEADS)))


def group(ref, g):
    return ref[pl.ds(pl.multiple_of(g * GH, GH), GH), :]


def tri_mask(upper):
    r = lax.broadcasted_iota(jnp.int32, (T, T), 0)
    c = lax.broadcasted_iota(jnp.int32, (T, T), 1)
    keep = (r <= c) if upper else (r >= c)
    return jnp.where(keep, 1.0, 0.0)


def neighbours():
    me = lax.axis_index(AXIS)
    core = lax.rem(me, 2)
    chip = lax.rem(me // 2, CHIPS)
    z = me // (2 * CHIPS)
    partner = me + 1 - 2 * core
    chips = [lax.rem(chip + r, CHIPS) for r in (2, 1, 3)]
    planes = [lax.rem(z + r, PLANES) for r in (1, 2, 3)]

    def at_chip(c):
        return me + 2 * (c - chip)

    def at_z(zz):
        return me + 2 * CHIPS * (zz - z)

    return core, chip, z, partner, chips, planes, at_chip, at_z


def greet(partner, chips, planes, at_chip, at_z):
    barrier = pltpu.get_barrier_semaphore()
    for p in [partner] + [at_chip(c) for c in chips] + [at_z(zz) for zz in planes]:
        pl.semaphore_signal(barrier, inc=1, device_id=(p,), device_id_type=MESH)


def met(chips, planes):
    pl.semaphore_wait(pltpu.get_barrier_semaphore(), 1 + len(chips) + len(planes))


def rcopy(src, dst, ssem, rsem, dev):
    return pltpu.make_async_remote_copy(src_ref=src, dst_ref=dst, send_sem=ssem, recv_sem=rsem,
                                        device_id=(dev,), device_id_type=MESH)


def each(copies, act):
    for cp in copies:
        getattr(cp, act)()


def link_steps(ng, sp, dsp, ld, s_init, ds_last, start, end, first, sp_out,
               r_s, r_ds, r_ld, c_s, c_ds, c_ld, p_s, p_ds, p_ld, t_s, t_ds, t_ld, z_b, z_ld,
               b_s, b_ds, a_s, a_ds, n_s, n_ds, f_own, f_all,
               send0, recv0, send1, recv1, send2, recv2, send3, recv3, send4, recv4, send5, recv5, loc):
    core, chip, z, partner, chips, planes, at_chip, at_z = neighbours()
    mine, theirs = core * SHARE, (1 - core) * SHARE

    def hello():
        greet(partner, chips, planes, at_chip, at_z)

    def own_loads(q):
        part = pl.ds(q * PIECE + mine + chip * OWN, OWN)
        return [pltpu.make_async_copy(s_init.at[part], b_s.at[q, 0], loc.at[q, 0]),
                pltpu.make_async_copy(ds_last.at[part], b_ds.at[q, CHIPS - 1], loc.at[q, 1])]

    def copies0(q):
        part = pl.ds(q * PIECE + theirs, SHARE)
        logs = pl.ds(q * PIECE, PIECE)
        return [rcopy(sp.at[part], r_s.at[q], send0.at[q, 0], recv0.at[q, 0], partner),
                rcopy(dsp.at[part], r_ds.at[q], send0.at[q, 1], recv0.at[q, 1], partner),
                rcopy(ld.at[logs], r_ld.at[q], send0.at[q, 2], recv0.at[q, 2], partner)]

    def swap(q):
        if q == 0:
            met(chips, planes)
        each(copies0(q) + own_loads(q), "start")

    def copies1(q, c_dst, c_slot):
        part = pl.ds(c_dst * OWN, OWN)
        dev = at_chip(c_dst)
        return [rcopy(c_ld.at[q], p_ld.at[q, c_slot], send1.at[q, 2, c_dst], recv1.at[q, 2, c_slot], dev),
                rcopy(c_s.at[q, part], p_s.at[q, c_slot], send1.at[q, 0, c_dst], recv1.at[q, 0, c_slot], dev),
                rcopy(c_ds.at[q, part], p_ds.at[q, c_slot], send1.at[q, 1, c_dst], recv1.at[q, 1, c_slot], dev)]

    def decay(ref, q, h):
        return jnp.exp2(ref[q, pl.ds(h, 1), :])

    def by_core(q, lower, upper):
        for k, run in enumerate((lower, upper)):
            @pl.when(core == k)
            def _():
                for h in range(SHARE):
                    hh = q * PIECE + mine + h
                    run(h, hh, jnp.exp2(ld[pl.ds(hh, 1), :]), decay(r_ld, q, mine + h))

    def pairs(q):
        each(copies0(q), "wait")
        c_ld[q] = ld[blk(q, PIECE), :] + r_ld[q]

        def join_lower(h, hh, own, oth):
            c_s[q, h] = sp[hh] * oth + r_s[q, h]
            c_ds[q, h] = dsp[hh] + own * r_ds[q, h]

        def join_upper(h, hh, own, oth):
            c_s[q, h] = r_s[q, h] * own + sp[hh]
            c_ds[q, h] = r_ds[q, h] + oth * dsp[hh]

        by_core(q, join_lower, join_upper)
        for c in chips:
            each(copies1(q, c, chip), "start")
        p_ld[q, chip] = c_ld[q]

        for h in range(OWN):
            p_s[q, chip, h] = c_s[q, chip * OWN + h]
            p_ds[q, chip, h] = c_ds[q, chip * OWN + h]

    def copy2(q, kind, z_dst, z_slot):
        return rcopy((t_s, t_ds)[kind].at[q], z_b.at[q, z_slot], send2.at[q, 0, z_dst], recv2.at[q, 0, z_slot], at_z(z_dst))

    def copy2_ld(q, z_dst, z_slot):
        return rcopy(t_ld.at[q], z_ld.at[q, z_slot], send2.at[q, 1, z_dst], recv2.at[q, 1, z_slot], at_z(z_dst))

    def chip_decays(q, h):
        return [jnp.exp2(p_ld[q, c, pl.ds(mine + chip * OWN + h, 1), :]) for c in ALL_CHIPS]

    def z_decay(q, zz, h):
        return jnp.exp2(z_ld[q, zz, pl.ds(mine + chip * OWN + h, 1), :])

    def plane(q):
        for c in chips:
            each(copies1(q, c, c), "wait_recv")
        t_ld[q] = sum(p_ld[q, c] for c in ALL_CHIPS)

        for h in range(OWN):
            d = chip_decays(q, h)
            acc = p_s[q, 0, h]
            for c in ALL_CHIPS[1:]:
                acc = acc * d[c] + p_s[q, c, h]
            t_s[q, h] = acc
            acc = p_ds[q, CHIPS - 1, h]
            for c in ALL_CHIPS[-2::-1]:
                acc = acc * d[c] + p_ds[q, c, h]
            t_ds[q, h] = acc

        for zz in planes:
            copy2_ld(q, zz, z).start()

            @pl.when(zz > z)
            def _():
                copy2(q, 0, zz, z).start()

            @pl.when(zz < z)
            def _():
                copy2(q, 1, zz, z).start()

    def copies3(q, c_dst, c_slot):
        dev = at_chip(c_dst)
        part = pl.ds(c_slot * OWN, OWN)
        return [rcopy(b_s.at[q, c_dst], a_s.at[q, part], send3.at[q, 0, c_dst], recv3.at[q, 0, c_slot], dev),
                rcopy(b_ds.at[q, c_dst], a_ds.at[q, part], send3.at[q, 1, c_dst], recv3.at[q, 1, c_slot], dev)]

    def copy_f(q, zz):
        return rcopy(f_own.at[q], f_all.at[q, pl.ds(chip * OWN, OWN)], send5.at[q, 0, zz], recv5.at[q, 0, chip], at_z(zz))

    def prefix(q):
        for zz in planes:
            copy2_ld(q, zz, zz).wait_recv()
            copy2(q, 0, zz, zz).wait_recv()
        each(own_loads(q), "wait")

        for zz in range(PLANES - 1):
            @pl.when(zz < z)
            def _():
                for h in range(OWN):
                    b_s[q, 0, h] = b_s[q, 0, h] * z_decay(q, zz, h) + z_b[q, zz, h]
        for zz in range(PLANES)[:0:-1]:
            @pl.when(zz > z)
            def _():
                for h in range(OWN):
                    b_ds[q, CHIPS - 1, h] = b_ds[q, CHIPS - 1, h] * z_decay(q, zz, h) + z_b[q, zz, h]
        for h in range(OWN):
            d = chip_decays(q, h)
            acc = b_s[q, 0, h]
            for c in ALL_CHIPS[:-1]:
                acc = acc * d[c] + p_s[q, c, h]
                b_s[q, c + 1, h] = acc
            acc = b_ds[q, CHIPS - 1, h]
            for c in ALL_CHIPS[:0:-1]:
                acc = acc * d[c] + p_ds[q, c, h]
                b_ds[q, c - 1, h] = acc
            f_own[q, h] = acc * d[0] + p_ds[q, 0, h]
            a_s[q, chip * OWN + h] = b_s[q, chip, h]
            a_ds[q, chip * OWN + h] = b_ds[q, chip, h]

        for c in chips:
            each(copies3(q, c, chip), "start")

    def send_first():
        @pl.when(z == 0)
        def _():
            for q in range(QS):
                for zz in range(1, PLANES):
                    copy_f(q, zz).start()

                @pl.loop(0, OWN)
                def _(h):
                    f_all[q, chip * OWN + h] = f_own[q, h]

    def out_copies(q, far_s, far_ds, near_s, near_ds):
        part = pl.ds(q * PIECE + mine, SHARE)
        return [rcopy(far_s.at[q], start.at[part], send4.at[q, 0], recv4.at[q, 0], partner),
                rcopy(far_ds.at[q], end.at[part], send4.at[q, 1], recv4.at[q, 1], partner),
                pltpu.make_async_copy(near_s.at[q], start.at[part], loc.at[q, 2]),
                pltpu.make_async_copy(near_ds.at[q], end.at[part], loc.at[q, 3])]

    def halve(q):
        for c in chips:
            each(copies3(q, c, c), "wait_recv")

        def lower(h, hh, own, oth):
            n_s[q, h] = own * a_s[q, h] + sp[hh]
            n_ds[q, h] = r_ds[q, h] + oth * a_ds[q, h]

        def upper(h, hh, own, oth):
            n_s[q, h] = oth * a_s[q, h] + r_s[q, h]
            n_ds[q, h] = dsp[hh] + own * a_ds[q, h]

        by_core(q, lower, upper)

        @pl.when(core == 0)
        def _():
            each(out_copies(q, n_s, a_ds, a_s, n_ds), "start")

        @pl.when(core == 1)
        def _():
            each(out_copies(q, a_s, n_ds, n_s, a_ds), "start")

    def copy5(q, c_dst, c_slot):
        part = f_all.at[q, pl.ds(c_slot * OWN, OWN)]
        return rcopy(part, part, send5.at[q, 1, c_dst], recv5.at[q, 1, c_slot], at_chip(c_dst))

    def spread(q):
        @pl.when(z > 0)
        def _():
            copy_f(q, z).wait_recv()

        for c in chips:
            copy5(q, c, chip).start()

    def last(q):
        part = first.at[pl.ds(q * PIECE + mine, SHARE)]
        return [rcopy(f_all.at[q], part, send4.at[q, 2], recv4.at[q, 2], partner),
                pltpu.make_async_copy(f_all.at[q], part, loc.at[q, 4])]

    def sp_copy():
        return [pltpu.make_async_copy(sp, sp_out, loc.at[0, 5])]

    def finish():
        for q in range(QS):
            for c in chips:
                copy5(q, c, c).wait_recv()
            each(last(q), "start")
        for q in range(QS):
            each(out_copies(q, n_s, a_ds, a_s, n_ds), "wait")
            for c in chips:
                each(copies1(q, c, chip) + copies3(q, c, chip) + [copy5(q, c, chip)], "wait_send")
            for zz in planes:
                copy2(q, 0, zz, z).wait_send()
                copy2_ld(q, zz, z).wait_send()

            @pl.when(z == 0)
            def _():
                for zz in range(1, PLANES):
                    copy_f(q, zz).wait_send()
        each(sp_copy(), "wait")
        for q in range(QS):
            each(last(q), "wait")

    early = {0: [hello], 4: [functools.partial(swap, 0)], 6: [functools.partial(pairs, 0)],
             8: [functools.partial(swap, 1), lambda: each(sp_copy(), "start")]}
    late = [(0, 1, functools.partial(pairs, 1)), (1, 3, functools.partial(plane, 0)), (3, 0, functools.partial(plane, 1)), (3, 3, functools.partial(prefix, 0)), (4, 5, functools.partial(prefix, 1)), (4, 5, send_first), (5, 2, functools.partial(halve, 0)), (6, 4, functools.partial(halve, 1)), (6, 4, functools.partial(spread, 0)), (7, 0, functools.partial(spread, 1)), (7, 5, finish)]
    return early, late


def link_shapes():
    st = (HD, N)
    V = pltpu.VMEM
    D = pltpu.SemaphoreType.DMA

    def states(*lead):
        return V((QS,) + lead + st, F32)

    def logs(*lead):
        return V((QS,) + lead + (PIECE, N), F32)

    share, four, own = states(SHARE), states(CHIPS, OWN), states(OWN)
    three = D((QS, 3, CHIPS))
    two = D((QS, 2, CHIPS))
    return [share, share, logs(), share, share, logs(), four, four, logs(CHIPS), own, own, logs(), four, logs(PLANES),
            four, four, share, share, share, share, own, share,
            D((QS, 3)), D((QS, 3)), three, three, two, two, two, two, D((QS, 3)), D((QS, 3)), two, two, D((QS, 6))]


def local_kernel(nb, ng, x_ref, dy_ref, dt_ref, alog_ref, b_ref, c_ref, s_init, ds_last,
                 du_ref, ry_ref, db_ref, dc_ref, cum_out, start, end, first, sp_out,
                 gram, dgram, s_cur, ds_cur, xw, yw, y_in, u_in, rcol, cums, rates, sp, dsp, ld, *link_scratch):
    step_id = pl.program_id(0)
    early, late = link_steps(ng, sp, dsp, ld, s_init, ds_last, start, end, first, sp_out, *link_scratch)
    for at, steps in early.items():
        @pl.when(step_id == at)
        def _():
            for step in steps:
                step()

    @pl.when(step_id == 0)
    def _():
        columns(rates, -jnp.exp(alog_ref[...]) * LOG2E)

    @pl.when(step_id < ng)
    def _():
        range_states(nb, step_id, x_ref, dy_ref, dt_ref, group(rates, step_id), b_ref, c_ref, cum_out, cums, sp, dsp, ld, xw, yw)

    @pl.when(step_id >= ng)
    def _():
        local_group(nb, ng, step_id - ng, late, x_ref, dy_ref, dt_ref, b_ref, c_ref, du_ref, ry_ref, db_ref, dc_ref,
                    gram, dgram, s_cur, ds_cur, xw, yw, y_in, u_in, rcol, cums.at[step_id - ng])


def range_states(nb, g, x_ref, dy_ref, dt_ref, rate, b_ref, c_ref, cum_out, cums, sp, dsp, ld, xw, yw):
    tri = tri_mask(True).astype(BF16)
    dt = dt_ref[...]
    a = dt * rate[:, :1]
    cum, before = [], [jnp.zeros((GH, 1), F32)]
    for i in range(nb):
        v = dot_tri(a[:, blk(i, T)], tri)
        cums[g, :, blk(i, T)] = v
        cum_out[:, blk(i, T)] = v
        cum.append(v)
        before.append(before[-1] + last_col(v))
    ld[pl.ds(pl.multiple_of(g * GH, GH), GH), :] = jnp.broadcast_to(before[nb], (GH, T))
    after = jnp.zeros((GH, 1), F32)
    acc_s = jnp.zeros((GR, N), F32)
    acc_ds = jnp.zeros((GR, N), F32)
    for i in reversed(range(nb)):
        tok = blk(i, T)
        w_in = dt[:, tok] * jnp.exp2((last_col(cum[i]) - cum[i]) + after)
        w_out = jnp.exp2(cum[i] + before[i])
        after = after + last_col(cum[i])
        for j in range(GH):
            rows = blk(j, HD)
            xw[i, rows, :T], xw[i, rows, T:] = split2(x_ref[rows, tok].astype(F32) * row(w_in, j))
            yw[i, rows, :T], yw[i, rows, T:] = split2(dy_ref[rows, tok].astype(F32) * row(w_out, j))
        acc_s += mm(xw[i], cat0(b_ref[tok, :], b_ref[tok, :]))
        acc_ds += mm(yw[i], cat0(c_ref[tok, :], c_ref[tok, :]))
    for j in range(GH):
        sp[g * GH + j] = acc_s[blk(j, HD), :]
        dsp[g * GH + j] = acc_ds[blk(j, HD), :]


def carry(state, weighted, k, other, tot, first):
    upd = mm(weighted[k], cat0(other, other))
    if first:
        state[...] = upd
        return
    decay = jnp.exp2(tot)
    for j in range(GH):
        rows = blk(j, HD)
        state[rows, :] = state[rows, :] * row(decay, j) + upd[rows, :]


def local_group(nb, ng, g, late, x_ref, dy_ref, dt_ref, b_ref, c_ref, du_ref, ry_ref, db_ref, dc_ref,
                gram, dgram, s_cur, ds_cur, xw, yw, y_in, u_in, rcol, cum_ref):
    @pl.when(g == 0)
    def _():
        low = tri_mask(False)
        for i in range(nb):
            tok = blk(i, T)
            gram[i] = mm_nt(c_ref[tok, :], b_ref[tok, :]) * low
            dgram[i] = jnp.zeros((T, T), F32)
        db_ref[...] = jnp.zeros_like(db_ref)
        dc_ref[...] = jnp.zeros_like(dc_ref)
        rcol[...] = jnp.zeros_like(rcol)

    @pl.loop(0, nb)
    def _(i):
        tok = pl.ds(pl.multiple_of(i * T, T), T)
        cum = cum_ref[:, tok]
        w_in = dt_ref[:, tok] * jnp.exp2(last_col(cum) - cum)
        e_out = jnp.exp2(cum)
        for j in range(GH):
            rows = blk(j, HD)
            hi, lo = split2(x_ref[rows, tok].astype(F32) * row(w_in, j))
            xw[i, rows, :T] = hi
            xw[i, rows, T:] = lo
            hi, lo = split2(dy_ref[rows, tok].astype(F32) * row(e_out, j))
            yw[i, rows, :T] = hi
            yw[i, rows, T:] = lo
            du_ref[rows, tok] = jnp.zeros((HD, T), F32)

    def block(i, first):
        for at_g, at_i, step in late:
            if (at_i == 0) == first:
                pl.when((g == at_g) if first else (g == at_g) & (i == at_i))(step)

        k = nb - 1 - i
        tok_k, tok = (blk(k, T), blk(i, T)) if first else (pl.ds(pl.multiple_of(k * T, T), T), pl.ds(pl.multiple_of(i * T, T), T))

        cum_k = cum_ref[:, tok_k]
        tot_k = last_col(cum_k)
        b_k = b_ref[tok_k, :]
        c_k = c_ref[tok_k, :]
        if not first:
            ds_hi, ds_lo = split2(ds_cur[...])
            u_in[...] = mm_nt(cat1(ds_hi, ds_lo), cat1(b_k, b_k))
            db2 = mm_tn(xw[k, :, :T], cat1(ds_hi, ds_lo))
            db_ref[tok_k, :] += db2[:, :N] + db2[:, N:] + mm_tn(xw[k, :, T:], ds_hi)
            e_in = jnp.exp2(tot_k - cum_k)
            for j in range(GH):
                rows = blk(j, HD)
                du_ref[rows, tok_k] += u_in[rows, :] * row(e_in, j)
        carry(ds_cur, yw, k, c_k, tot_k, first)

        cum = cum_ref[:, tok]
        e_out = jnp.exp2(cum)
        dt = dt_ref[:, tok]
        b_i = b_ref[tok, :]
        c_i = c_ref[tok, :]
        if not first:
            s_hi, s_lo = split2(s_cur[...])
            y_in[...] = mm_nt(cat1(s_hi, s_lo), cat1(c_i, c_i))
            dc2 = mm_tn(yw[i, :, :T], cat1(s_hi, s_lo))
            dc_ref[tok, :] += dc2[:, :N] + dc2[:, N:] + mm_tn(yw[i, :, T:], s_hi)
        carry(s_cur, xw, i, b_i, last_col(cum), first)
        cum_c = jnp.transpose(cum)
        g_i = gram[i]
        zero = jnp.zeros((HD, T), BF16)
        inter = []
        for j0 in range(0, GH, 2):
            y_t = jnp.transpose(dy_ref[pl.ds(j0 * HD, T), tok])
            u0, v0 = split2(x_ref[blk(j0, HD), tok].astype(F32) * row(dt, j0))
            u1, v1 = split2(x_ref[blk(j0 + 1, HD), tok].astype(F32) * row(dt, j0 + 1))
            pair = mm(cat1(y_t, y_t), cat1(cat0(u0, zero, v0, zero), cat0(zero, u1, zero, v1)))
            e_sum = None
            for j, p in ((j0, pair[:, :T]), (j0 + 1, pair[:, T:])):
                rows = blk(j, HD)
                lam = jnp.exp2(jnp.minimum(cum_c[:, blk(j, 1)] - row(cum, j), 0.0))
                e_sum = lam * p if e_sum is None else e_sum + lam * p
                m = lam * g_i
                rcol[:, blk(j, 1)] = sum1(m * p)
                m_hi, m_lo = split2(m)
                yb = dy_ref[rows, tok]
                du_ref[rows, tok] += mm(cat1(yb, yb), cat0(m_hi, m_lo))
                if not first:
                    inter.append(sum0(yb.astype(F32) * y_in[rows, :]))
            dgram[i] += e_sum
        own = jnp.transpose(rcol[...])[:GH, :]
        ry_ref[:, tok] = own + e_out * cat0(*inter) if inter else own

    block(0, True)

    @pl.loop(1, nb)
    def _(i):
        block(i, False)

    @pl.when(g == ng - 1)
    def _():
        low_f = tri_mask(False)
        for i in range(nb):
            tok = blk(i, T)
            bb = b_ref[tok, :]
            cc = c_ref[tok, :]
            hi, lo = split2(dgram[i] * low_f)
            dc_ref[tok, :] += mm(hi, bb) + mm(lo, bb)
            db_ref[tok, :] += mm_tn(hi, cc) + mm_tn(lo, cc)


def local_grads(x_t, dy_t, dt_t, a_log, b, c, s_init, ds_last):
    rows, seq = x_t.shape
    nb, ng = seq // T, rows // GR
    big = pl.BlockSpec((GR, seq), lambda g: (lax.rem(g, ng), 0))
    head = pl.BlockSpec((GH, seq), lambda g: (lax.rem(g, ng), 0))
    per_head = pl.BlockSpec((1, HEADS), lambda g: (0, 0))
    big_o = pl.BlockSpec((GR, seq), lambda g: (jnp.maximum(g - ng, 0), 0))
    head_o = pl.BlockSpec((GH, seq), lambda g: (jnp.maximum(g - ng, 0), 0))
    cum_o = pl.BlockSpec((GH, seq), lambda g: (jnp.minimum(g, ng - 1), 0))
    full = pl.BlockSpec((seq, N), lambda g: (0, 0))
    anyw = pl.BlockSpec(memory_space=pl.ANY)
    sd = jax.ShapeDtypeStruct
    state = sd((HEADS, HD, N), F32)
    V = pltpu.VMEM
    sq, grp, wide = V((nb, T, T), F32), V((GR, N), F32), V((nb, GR, 2 * T), BF16)
    return pl.pallas_call(
        functools.partial(local_kernel, nb, ng),
        grid=(2 * ng,),
        in_specs=[big, big, head, per_head, full, full, anyw, anyw],
        out_specs=[big_o, head_o, full, full, cum_o, anyw, anyw, anyw, anyw],
        out_shape=[sd((rows, seq), F32), sd((rows // HD, seq), F32), sd((seq, N), F32), sd((seq, N), F32),
                   sd((rows // HD, seq), F32), state, state, state, state],
        scratch_shapes=[sq, sq, grp, grp, wide, wide, grp, grp, V((T, T), F32), V((ng, GH, seq), F32),
                        V((HEADS, T), F32),
                        V((HEADS, HD, N), F32), V((HEADS, HD, N), F32), V((HEADS, N), F32)] + link_shapes(),
        compiler_params=pltpu.CompilerParams(dimension_semantics=("arbitrary",), collective_id=0, has_side_effects=True),
        name="local_grads",
    )(x_t, dy_t, dt_t, a_log, b, c, s_init, ds_last)


T2 = 256


def join_kernel(nb, ng, x_ref, dy_ref, dt_ref, cum_ref, alog_ref, dskip_ref, s0_ref, dse_ref, sp_ref, b_ref, c_ref,
                du_ref, ry_ref, dbl_ref, dcl_ref, f_ref,
                dx_ref, ddt_ref, dal_ref, dsk_ref, db_ref, dc_ref, first_ref,
                rates, skips, db_acc, dc_acc, ein, eout, xw, yw, s2, d2, y_in, u_in, dcum, xdu, skt):
    g = pl.program_id(0)

    @pl.when(g == 0)
    def _():
        db_acc[...] = dbl_ref[...]
        dc_acc[...] = dcl_ref[...]
        columns(rates, -jnp.exp(alog_ref[...]))
        columns(skips, dskip_ref[...])

    first_ref[...] = f_ref[...]
    rate = group(rates, g)
    skip = group(skips, g)[:, :1]
    cums = [cum_ref[:, i * T:(i + 1) * T] for i in range(nb)]
    tots = [last_col(v) for v in cums]
    acc = jnp.zeros_like(tots[0])
    for i in range(nb):
        eout[:, i * T:(i + 1) * T] = jnp.exp2(cums[i] + acc)
        acc = acc + tots[i]
    e_tot = jnp.exp2(acc)
    acc = jnp.zeros_like(tots[0])
    for i in reversed(range(nb)):
        ein[:, i * T:(i + 1) * T] = jnp.exp2((tots[i] - cums[i]) + acc)
        acc = acc + tots[i]

    s_hi, s_lo = split2(s0_ref[...])
    d_hi, d_lo = split2(dse_ref[...])
    s2[...] = cat1(s_hi, s_lo)
    d2[...] = cat1(d_hi, d_lo)

    for i in range(nb * T // T2):
        tok = blk(i, T2)
        bb = b_ref[tok, :]
        cc = c_ref[tok, :]
        y_in[...] = mm_nt(s2[...], cat1(cc, cc))
        u_in[...] = mm_nt(d2[...], cat1(bb, bb))
        dt = dt_ref[:, tok]
        e_in = ein[:, tok]
        e_out = eout[:, tok]
        w_in = dt * e_in
        xds, rys, sks = [], [], []
        for j in range(GH):
            rows = blk(j, HD)
            xf = x_ref[rows, tok].astype(F32)
            yf = dy_ref[rows, tok].astype(F32)
            du = du_ref[rows, tok] + row(e_in, j) * u_in[rows, :]
            dx_ref[rows, tok] = (row(dt, j) * du + row(skip, j) * yf).astype(BF16)
            xds.append(sum0(xf * du))
            rys.append(sum0(yf * y_in[rows, :]))
            sks.append(sum0(xf * yf))
            xw[rows, :T2], xw[rows, T2:] = split2(xf * row(w_in, j))
            yw[rows, :T2], yw[rows, T2:] = split2(yf * row(e_out, j))
        dc2 = mm_tn(yw[:, :T2], s2[...])
        dc_acc[tok, :] += dc2[:, :N] + dc2[:, N:] + mm_tn(yw[:, T2:], s2[:, :N])
        db2 = mm_tn(xw[:, :T2], d2[...])
        db_acc[tok, :] += db2[:, :N] + db2[:, N:] + mm_tn(xw[:, T2:], d2[:, :N])
        xd = cat0(*xds)
        xdu[:, tok] = xd
        dcum[:, tok] = ry_ref[:, tok] + e_out * cat0(*rys) - dt * xd
        skt[:, tok] = cat0(*sks)

    for j in range(GH):
        rows = blk(j, HD)
        dal_ref[j:j + 1, :] = jnp.sum(dse_ref[rows, :] * (sp_ref[rows, :] + row(e_tot, j) * s0_ref[rows, :]), axis=0, keepdims=True)
    run = jnp.sum(dal_ref[...], axis=1, keepdims=True)
    low = tri_mask(False).astype(BF16)
    total = jnp.zeros((GH, T), F32)
    for i in reversed(range(nb)):
        tok = blk(i, T)
        da = dot_tri(dcum[:, tok], low) + run
        run = da[:, 0:1]
        da = da * rate
        ddt_ref[:, tok] = xdu[:, tok] + da
        total = total + dt_ref[:, tok] * da
    dal_ref[...] = jnp.broadcast_to(jnp.sum(total, axis=1, keepdims=True), (GH, T))
    dsk_ref[...] = jnp.broadcast_to(jnp.sum(skt[...], axis=1, keepdims=True), (GH, T))

    @pl.when(g == ng - 1)
    def _():
        db_ref[...] = db_acc[...].astype(BF16)
        dc_ref[...] = dc_acc[...].astype(BF16)


def join_grads(x_t, dy_t, dt_t, cum, a_log, d_skip, s0, dse, sp, b, c, du, ry, dbl, dcl, first):
    rows, seq = x_t.shape
    nb, ng = seq // T, rows // GR
    big = pl.BlockSpec((GR, seq), lambda g: (g, 0))
    head = pl.BlockSpec((GH, seq), lambda g: (g, 0))
    hd1 = pl.BlockSpec((GH, T), lambda g: (g, 0))
    per_head = pl.BlockSpec((1, HEADS), lambda g: (0, 0))
    full = pl.BlockSpec((seq, N), lambda g: (0, 0))
    st = pl.BlockSpec((GR, N), lambda g: (g, 0))
    sd = jax.ShapeDtypeStruct
    return pl.pallas_call(
        functools.partial(join_kernel, nb, ng),
        grid=(ng,),
        in_specs=[big, big, head, head, per_head, per_head, st, st, st, full, full, big, head, full, full, st],
        out_specs=[big, head, hd1, hd1, full, full, st],
        out_shape=[sd((rows, seq), BF16), sd((rows // HD, seq), F32), sd((rows // HD, T), F32),
                   sd((rows // HD, T), F32), sd((seq, N), BF16), sd((seq, N), BF16), sd((rows, N), F32)],
        scratch_shapes=[pltpu.VMEM((HEADS, T), F32), pltpu.VMEM((HEADS, T), F32),
                        pltpu.VMEM((seq, N), F32), pltpu.VMEM((seq, N), F32),
                        pltpu.VMEM((GH, seq), F32), pltpu.VMEM((GH, seq), F32),
                        pltpu.VMEM((GR, 2 * T2), BF16), pltpu.VMEM((GR, 2 * T2), BF16),
                        pltpu.VMEM((GR, 2 * N), BF16), pltpu.VMEM((GR, 2 * N), BF16),
                        pltpu.VMEM((GR, T2), F32), pltpu.VMEM((GR, T2), F32),
                        pltpu.VMEM((GH, seq), F32), pltpu.VMEM((GH, seq), F32), pltpu.VMEM((GH, seq), F32)],
        compiler_params=pltpu.CompilerParams(dimension_semantics=("arbitrary",)),
        name="join_grads",
    )(x_t, dy_t, dt_t, cum, a_log, d_skip, s0, dse, sp, b, c, du, ry, dbl, dcl, first)

HALF_ROWS = GH // 2
IN_PLANE = 2 * CHIPS


def sum_kernel(dal_ref, dsk_ref, out_ref, v1, v2, send, recv):
    me = lax.axis_index(AXIS)
    pos, z = lax.rem(me, IN_PLANE), me // IN_PLANE
    near = [lax.rem(pos + r, IN_PLANE) for r in range(1, IN_PLANE)]
    far = [lax.rem(z + r, PLANES) for r in range(1, PLANES)]

    def at_pos(o):
        return me + o - pos

    def at_z(o):
        return me + IN_PLANE * (o - z)

    barrier = pltpu.get_barrier_semaphore()
    for p in [at_pos(o) for o in near] + [at_z(o) for o in far]:
        pl.semaphore_signal(barrier, inc=1, device_id=(p,), device_id_type=MESH)
    v1[pos] = cat0(jnp.transpose(dal_ref[...])[:HALF_ROWS, :], jnp.transpose(dsk_ref[...])[:HALF_ROWS, :])
    pl.semaphore_wait(barrier, len(near) + len(far))

    def exchange(buf, stage, own, others, at):
        def copy(to, slot, dev):
            return rcopy(buf.at[slot], buf.at[slot], send.at[stage, to], recv.at[stage, slot], dev)

        each([copy(o, own, at(o)) for o in others], "start")
        each([copy(o, o, at(o)) for o in others], "wait_recv")
        each([copy(o, own, at(o)) for o in others], "wait_send")

    exchange(v1, 0, pos, near, at_pos)
    v2[z] = sum(v1[o] for o in range(IN_PLANE))
    exchange(v2, 1, z, far, at_z)
    out_ref[...] = sum(v2[o] for o in range(PLANES))


def sum_devices(dal, dsk):
    vm = pl.BlockSpec(memory_space=pltpu.VMEM)
    out = pl.pallas_call(
        sum_kernel,
        in_specs=[vm, vm],
        out_specs=vm,
        out_shape=jax.ShapeDtypeStruct((GH, HEADS), F32),
        scratch_shapes=[pltpu.VMEM((IN_PLANE, GH, HEADS), F32), pltpu.VMEM((PLANES, GH, HEADS), F32),
                        pltpu.SemaphoreType.DMA((2, IN_PLANE)), pltpu.SemaphoreType.DMA((2, IN_PLANE))],
        compiler_params=pltpu.CompilerParams(collective_id=1, has_side_effects=True),
        name="sum_devices",
    )(dal, dsk)
    return out[0], out[HALF_ROWS]


def solution(mesh):
    tok4 = P(None, AXIS, None, None)
    tok3 = P(None, AXIS, None)

    def device_step(x_loc, dt_loc, a_log, b_loc, c_loc, d_skip, s_init, dy_loc, ds_last):
        seq = x_loc.shape[1]
        x_t = x_loc[0].transpose(1, 2, 0).reshape(HEADS * HD, seq)
        dy_t = dy_loc[0].transpose(1, 2, 0).reshape(HEADS * HD, seq)
        dt_t = dt_loc[0].T
        a_row, d_row = a_log[None], d_skip[None]
        b, c = b_loc[0], c_loc[0]
        flat = (HEADS * HD, N)
        du, ry, dbl, dcl, cum, start, end, first, sp = local_grads(x_t, dy_t, dt_t, a_row, b, c, s_init[0], ds_last[0])
        dx, ddt, dal, dsk, db, dc, ds_first = join_grads(x_t, dy_t, dt_t, cum, a_row, d_row, start.reshape(flat),
                                                         end.reshape(flat), sp.reshape(flat), b, c, du, ry, dbl, dcl,
                                                         first.reshape(flat))
        grad_x = dx.reshape(HEADS, HD, seq).transpose(2, 0, 1)[None]
        grad_alog, grad_skip = sum_devices(dal, dsk)
        return grad_x, ddt.T[None], db[None], dc[None], ds_first.reshape(HEADS, HD, N)[None], grad_alog, grad_skip

    return jax.shard_map(device_step, mesh=mesh,
                         in_specs=(tok4, tok3, P(), tok3, tok3, P(), P(), tok4, P()),
                         out_specs=(tok4, tok3, tok3, tok3, P(), P(), P()),
                         check_vma=False)
```
